32 devices in a mesh: seq: 8 (over z, y), head: 4 (over x, core).
Axes of the slice: x: 2, y: 2, z: 4, core: 2. Of those that a mesh axis runs over, the one named last changes fastest.
Arguments:
- queries: bfloat16 [2048, 8192], P('seq', 'head'), may hold values from -40 to 40
- key_rows: bfloat16 [2048, 8192], P('seq', 'head'), may hold values from -20 to 20
- value_rows: bfloat16 [2048, 8192], P('seq', 'head'), may hold values from -8 to 8
Outputs:
- attended: bfloat16 [2048, 8192], P('seq', 'head')
The draws below stay inside these ranges and needn't reach their ends.
All inputs are finite; a program needn't handle non-finite values.
Results may differ from the reference program's by a relative error of at most 0.0043.
Values may be sent and summed in bfloat16 or wider, within the bound.
A program may use at most 128 MiB of HBM per device.

```python
import math
from functools import reduce
import jax
import jax.numpy as jnp
from jax import lax

HEADS = 64
HEAD_DIM = 128
BLOCK = 128
POOL = 64
MID_REACH = 3
FAR_REACH = 9
TOKENS = 2048


def rough_field(folded, rows_total):
    return jax.random.truncated_normal(folded, -4.0, 4.0, (rows_total, HEADS * HEAD_DIM), jnp.float32)


def group_field(folded):
    group_part = jax.random.truncated_normal(folded, -4.0, 4.0, (TOKENS // POOL, HEADS * HEAD_DIM), jnp.float32)
    return jnp.repeat(group_part, POOL, axis=0)


def paired_keys(key):
    folded = jax.random.fold_in(key, 11)
    drawn = 3.0 * rough_field(jax.random.fold_in(folded, 1), TOKENS) + 1.5 * group_field(jax.random.fold_in(folded, 2))
    return drawn


def draw_key_rows(key, part):
    return paired_keys(key).astype(jnp.bfloat16)


def draw_queries(key, part):
    drawn = rough_field(jax.random.fold_in(key, 23), TOKENS)
    return drawn.astype(jnp.bfloat16)


def draw_value_rows(key, part):
    folded = jax.random.fold_in(key, 31)
    drawn = rough_field(jax.random.fold_in(folded, 1), TOKENS) + group_field(jax.random.fold_in(folded, 2))
    return drawn.astype(jnp.bfloat16)


def setup_inputs(seed: int = 0) -> dict:
    key_list = jax.random.split(jax.random.key(seed), 4)
    return {
        "queries": draw_queries(jax.random.fold_in(key_list[3], 71), 0),
        "key_rows": draw_key_rows(jax.random.fold_in(key_list[3], 71), 0),
        "value_rows": draw_value_rows(jax.random.fold_in(key_list[3], 71), 0),
    }


def pool_pairs(source):
    paired = source.astype(jnp.float32).reshape(source.shape[0] // 2, 2, source.shape[1])
    return (0.5 * (paired[:, 0] + paired[:, 1])).astype(jnp.bfloat16)

def pool_groups(source, group_rows):
    grouped = source.astype(jnp.float32).reshape(source.shape[0] // group_rows, group_rows, source.shape[1])
    return lax.optimization_barrier(jnp.mean(grouped, axis=1)).astype(jnp.bfloat16)

def padded(source, margin):
    return jnp.pad(source, ((margin, margin), (0, 0)))

def as_heads(source):
    return source.astype(jnp.float32).reshape(source.shape[0], HEADS, HEAD_DIM)

def reference(queries, key_rows, value_rows):
    score_scale = 1.0 / math.sqrt(HEAD_DIM)
    key_two = pool_pairs(key_rows)
    value_two = pool_pairs(value_rows)
    key_four = pool_pairs(key_two)
    value_four = pool_pairs(value_two)
    key_coarse = pool_groups(key_four, POOL // 4)
    value_coarse = pool_groups(value_four, POOL // 4)
    half_rows = BLOCK // 2
    quarter = BLOCK // 4
    blocks_all = TOKENS // BLOCK
    fine_pads = (padded(key_rows, BLOCK), padded(value_rows, BLOCK))
    mid_pads = (padded(key_two, MID_REACH * half_rows), padded(value_two, MID_REACH * half_rows))
    far_pads = (padded(key_four, FAR_REACH * quarter), padded(value_four, FAR_REACH * quarter))
    coarse_block = POOL * jnp.arange(TOKENS // POOL, dtype=jnp.int32) // BLOCK
    fine_span = 3 * BLOCK
    mid_span = (2 * MID_REACH + 1) * half_rows
    far_span = (2 * FAR_REACH + 1) * quarter

    def window(pads, anchor, span):
        return (lax.dynamic_slice_in_dim(pads[0], anchor, span, 0), lax.dynamic_slice_in_dim(pads[1], anchor, span, 0))

    def one_block(block_index):
        query_rows = as_heads(lax.dynamic_slice_in_dim(queries, block_index * BLOCK, BLOCK, 0))
        fine_pair = window(fine_pads, block_index * BLOCK, fine_span)
        mid_pair = window(mid_pads, block_index * half_rows, mid_span)
        far_pair = window(far_pads, block_index * quarter, far_span)
        fine_block = block_index - 1 + jnp.arange(fine_span, dtype=jnp.int32) // BLOCK
        mid_block = block_index - MID_REACH + jnp.arange(mid_span, dtype=jnp.int32) // half_rows
        far_block = block_index - FAR_REACH + jnp.arange(far_span, dtype=jnp.int32) // quarter
        level_list = [(fine_pair, fine_block, 0, 1, 0.0), (mid_pair, mid_block, 2, MID_REACH, math.log(2.0)), (far_pair, far_block, MID_REACH + 1, FAR_REACH, math.log(4.0)), ((key_coarse, value_coarse), coarse_block, FAR_REACH + 1, blocks_all, math.log(POOL))]
        score_list = []
        for pair_rows, atom_block, lowest, highest, log_size in level_list:
            gap_blocks = jnp.abs(atom_block - block_index)
            allowed = (atom_block >= 0) & (atom_block < blocks_all) & (gap_blocks >= lowest) & (gap_blocks <= highest)
            scores = jnp.einsum('qhe,khe->hqk', query_rows, as_heads(pair_rows[0])) * score_scale + log_size
            score_list.append(jnp.where(allowed[None, None, :], scores, -jnp.inf))
        row_top = reduce(jnp.maximum, [lax.optimization_barrier(jnp.max(scores, axis=2)) for scores in score_list])
        denominator = jnp.zeros((HEADS, BLOCK), jnp.float32)
        weighted = jnp.zeros((BLOCK, HEADS, HEAD_DIM), jnp.float32)
        for scores, level_item in zip(score_list, level_list):
            exp_terms = jnp.exp(scores - row_top[:, :, None])
            denominator = denominator + lax.optimization_barrier(jnp.sum(exp_terms, axis=2))
            rounded = lax.optimization_barrier(exp_terms.astype(jnp.bfloat16))
            weighted = weighted + jnp.einsum('hqk,khe->qhe', rounded.astype(jnp.float32), as_heads(level_item[0][1]))
        result = weighted / jnp.transpose(denominator)[:, :, None]
        return result.reshape(BLOCK, HEADS * HEAD_DIM).astype(jnp.bfloat16)
    blocks = lax.map(one_block, jnp.arange(blocks_all, dtype=jnp.int32))
    return blocks.reshape(TOKENS, HEADS * HEAD_DIM)
```

```python
import functools
import math

import jax
import jax.numpy as jnp
from jax import lax
from jax.experimental import pallas as pl
from jax.experimental.pallas import tpu as pltpu
from jax.sharding import PartitionSpec as P

HEAD_DIM = 128
BLOCK = 128
POOL = 64
MID_REACH = 3
FAR_REACH = 9

HALF = BLOCK // 2
QUARTER = BLOCK // 4
GROUP_BLOCKS = 4
GROUP_ROWS = GROUP_BLOCKS * BLOCK
COARSE_SLOT = 16
COARSE_USED = GROUP_ROWS // POOL

FINE_LOW, FINE_BLOCKS = -1, GROUP_BLOCKS + 2
MID_LOW, MID_BLOCKS = -MID_REACH, GROUP_BLOCKS + 2 * MID_REACH
FAR_LOW, FAR_BLOCKS = -FAR_REACH, GROUP_BLOCKS + 2 * FAR_REACH

KIND_K, KIND_V, KIND_Q, KIND_O, KIND_EDGE_K, KIND_EDGE_V, KIND_FINE, KIND_MID_OWN = range(8)
KIND_MID_OTHER, KIND_FAR = KIND_MID_OWN + 2, KIND_MID_OWN + 4
SECOND_HOP = (
    (13, 2, -4, 4, -8, 1),
    (14, -2, 4, 4, 8, -1),
)
DIRECT = (
    (15, 3, 3, 1, -9, 3),
    (16, -3, 0, 1, 12, -3),
)
RELAY_LAG, ATTEND_LAG = 3, 6
KINDS = 17
MESH = pl.DeviceIdType.MESH


def pool_matrix(out_rows, in_rows, group_rows):
    row = lax.broadcasted_iota(jnp.int32, (out_rows, in_rows), 0)
    col = lax.broadcasted_iota(jnp.int32, (out_rows, in_rows), 1)
    return jnp.where(col // group_rows == row, 1.0 / group_rows, 0.0).astype(jnp.bfloat16)


def pooled(source, out_rows, group_rows):
    weights = pool_matrix(out_rows, source.shape[0], group_rows)
    return jnp.dot(weights, source, preferred_element_type=jnp.float32).astype(jnp.bfloat16)


def kernel(
    groups, q_ref, k_ref, v_ref, o_ref,
    q_rows, fine, mid, far, coarse, out_rows, bias,
    send, recv, coarse_send, coarse_recv, local, entered,
):
    me = lax.axis_index("seq")
    group = me // 2
    parity = me % 2
    partner = me + 1 - 2 * parity
    outward = 2 * parity - 1
    rows_dev = q_ref.shape[0]
    chunks = q_rows.shape[0]
    half_cols = chunks * HEAD_DIM
    own_first = pl.multiple_of(parity * rows_dev, rows_dev)
    other_first = pl.multiple_of((1 - parity) * rows_dev, rows_dev)
    half_blocks = GROUP_BLOCKS // 2

    def own_cols(chunk):
        return pl.ds(pl.multiple_of(parity * half_cols + chunk * HEAD_DIM, HEAD_DIM), HEAD_DIM)

    def other_cols(chunk):
        return pl.ds(pl.multiple_of((1 - parity) * half_cols + chunk * HEAD_DIM, HEAD_DIM), HEAD_DIM)

    def fine_rows(block):
        return pl.ds(pl.multiple_of((block - FINE_LOW) * BLOCK, BLOCK), BLOCK)

    def remote(src, dst, kind, chunk, target):
        return pltpu.make_async_remote_copy(
            src_ref=src, dst_ref=dst, send_sem=send.at[chunk, kind], recv_sem=recv.at[chunk, kind],
            device_id={"seq": target}, device_id_type=MESH,
        )

    def exchange(kind, chunk):
        if kind == KIND_Q:
            return remote(
                q_ref.at[:, other_cols(chunk)], q_rows.at[chunk, pl.ds(own_first, rows_dev)],
                kind, chunk, partner,
            )
        if kind == KIND_O:
            return remote(
                out_rows.at[chunk, pl.ds(other_first, rows_dev)], o_ref.at[:, own_cols(chunk)],
                kind, chunk, partner,
            )
        source = k_ref if kind == KIND_K else v_ref
        return remote(
            source.at[:, other_cols(chunk)], fine.at[chunk, kind, pl.ds(BLOCK + own_first, rows_dev)],
            kind, chunk, partner,
        )

    def edge_copy(side, chunk):
        source = v_ref if side else k_ref
        rows = pl.ds(pl.multiple_of(parity * (rows_dev - BLOCK), BLOCK), BLOCK)
        landing = (1 - parity) * (GROUP_BLOCKS + 1) - 1
        return remote(
            source.at[rows, own_cols(chunk)], fine.at[chunk, side, fine_rows(landing)],
            KIND_EDGE_K + side, chunk, me + 2 * outward,
        )

    def fine_copy(chunk):
        first = (1 - parity) * (GROUP_BLOCKS - 1)
        landing = parity * (GROUP_BLOCKS + 1) - 1
        return remote(
            fine.at[chunk, :, fine_rows(first)], fine.at[chunk, :, fine_rows(landing)],
            KIND_FINE, chunk, me - 2 * outward,
        )

    def mid_rows(block):
        return pl.ds(pl.multiple_of((block - MID_LOW) * HALF, HALF), HALF)

    def far_rows(first, count):
        return pl.ds((first - FAR_LOW) * QUARTER, count * QUARTER)

    def mid_copy(other, way, chunk):
        block = 2 - parity if other else 1 + parity
        return remote(
            mid.at[chunk, :, mid_rows(block)], mid.at[chunk, :, mid_rows(block - GROUP_BLOCKS * way)],
            KIND_MID_OWN + 2 * other + (way < 0), chunk, me + 2 * way,
        )

    def far_copy(way, chunk):
        first, landing = (0, -GROUP_BLOCKS) if way > 0 else (GROUP_BLOCKS - 1, 2 * GROUP_BLOCKS - 1)
        return remote(
            far.at[chunk, :, far_rows(first, 1)], far.at[chunk, :, far_rows(landing, 1)],
            KIND_FAR + (way < 0), chunk, me + 2 * way,
        )

    def routed(route, chunk):
        kind, offset, first, count, landing, hop = route
        return remote(
            far.at[chunk, :, far_rows(first, count)], far.at[chunk, :, far_rows(landing, count)],
            kind, chunk, me + 2 * hop,
        )

    def coarse_copy(chunk, step):
        target = lax.rem(group + step, groups) * 2 + parity
        slot = pl.ds(pl.multiple_of(group * COARSE_SLOT, COARSE_SLOT), COARSE_SLOT)
        return pltpu.make_async_remote_copy(
            src_ref=coarse.at[chunk, :, slot], dst_ref=coarse.at[chunk, :, slot],
            send_sem=coarse_send.at[chunk, step], recv_sem=coarse_recv.at[chunk, step],
            device_id={"seq": target}, device_id_type=MESH,
        )

    def inside(offset):
        return (group + offset >= 0) & (group + offset < groups)

    def start_routes(routes, chunk):
        for route in routes:
            @pl.when(inside(route[5]) & inside(route[5] - route[1]))
            def _():
                routed(route, chunk).start()

    def await_routes(routes, chunk):
        for route in routes:
            @pl.when(inside(-route[1]))
            def _():
                routed(route, chunk).wait_recv()

    def own_copy(kind, chunk):
        if kind == KIND_Q:
            source, target = q_ref, q_rows.at[chunk, pl.ds(own_first, rows_dev)]
        else:
            source = k_ref if kind == KIND_K else v_ref
            target = fine.at[chunk, kind, pl.ds(BLOCK + own_first, rows_dev)]
        return pltpu.make_async_copy(source.at[:, own_cols(chunk)], target, local.at[chunk, kind])

    def own_result(chunk):
        return pltpu.make_async_copy(
            out_rows.at[chunk, pl.ds(own_first, rows_dev)], o_ref.at[:, own_cols(chunk)],
            local.at[chunk, KIND_O],
        )

    @pl.loop(0, chunks)
    def _(chunk):
        coarse[chunk] = jnp.zeros(coarse.shape[1:], jnp.bfloat16)

    barrier = pltpu.get_barrier_semaphore()
    pl.semaphore_signal(barrier, inc=1, device_id={"seq": partner}, device_id_type=MESH)
    for way in (1, -1):
        @pl.when(inside(way))
        def _():
            pl.semaphore_signal(barrier, inc=1, device_id={"seq": me + 2 * way}, device_id_type=MESH)

    pl.semaphore_wait(barrier, 1 + inside(1).astype(jnp.int32) + inside(-1).astype(jnp.int32))

    @pl.loop(0, chunks)
    def _(chunk):
        own_copy(KIND_K, chunk).start()
        own_copy(KIND_V, chunk).start()
        exchange(KIND_K, chunk).start()
        exchange(KIND_V, chunk).start()

        @pl.when(inside(outward))
        def _():
            edge_copy(0, chunk).start()
            edge_copy(1, chunk).start()

    @pl.loop(0, chunks)
    def _(chunk):
        own_copy(KIND_Q, chunk).start()
        exchange(KIND_Q, chunk).start()

    def pool_half(chunk, half):
        first = half * rows_dev
        for side in range(2):
            rows = fine[chunk, side, pl.ds(pl.multiple_of(BLOCK + first, BLOCK), rows_dev)]
            twos = pooled(rows, rows_dev // 2, 2)
            fours = pooled(twos, rows_dev // 4, 2)
            mid[chunk, side, pl.ds(pl.multiple_of(-MID_LOW * HALF + first // 2, HALF), rows_dev // 2)] = twos
            far[chunk, side, pl.ds(pl.multiple_of(-FAR_LOW * QUARTER + first // 4, QUARTER), rows_dev // 4)] = fours

    @pl.loop(0, chunks)
    def _(chunk):
        own_copy(KIND_K, chunk).wait()
        own_copy(KIND_V, chunk).wait()
        pool_half(chunk, parity)
        for way in (-1, 1):
            @pl.when(inside(way))
            def _():
                mid_copy(0, way, chunk).start()

                @pl.when(outward == -way)
                def _():
                    far_copy(way, chunk).start()

    for way in (1, -1):
        @pl.when(inside(-way))
        def _():
            pl.semaphore_wait(entered.at[(1 - way) // 2], 1)

        @pl.when(inside(way))
        def _():
            pl.semaphore_signal(
                entered.at[(1 - way) // 2], inc=1, device_id={"seq": me + 2 * way}, device_id_type=MESH
            )

    for window, unit, low, offset, landing, count in (
        (fine, BLOCK, FINE_LOW, 1, -1, 1),
        (fine, BLOCK, FINE_LOW, -1, 4, 1),
        (mid, HALF, MID_LOW, 1, -3, 2),
        (mid, HALF, MID_LOW, -1, 5, 2),
        (far, QUARTER, FAR_LOW, 1, -4, 1),
        (far, QUARTER, FAR_LOW, -1, 7, 1),
        (far, QUARTER, FAR_LOW, 2, -8, 4),
        (far, QUARTER, FAR_LOW, -2, 8, 4),
        (far, QUARTER, FAR_LOW, 3, -9, 1),
        (far, QUARTER, FAR_LOW, -3, 12, 1),
    ):
        @pl.when(jnp.logical_not(inside(-offset)))
        def _():
            @pl.loop(0, chunks)
            def _(chunk):
                window[chunk, :, pl.ds((landing - low) * unit, count * unit)] = jnp.zeros(
                    (2, count * unit, HEAD_DIM), jnp.bfloat16
                )

    atoms = bias.shape[1]
    total_blocks = groups * GROUP_BLOCKS
    place = lax.broadcasted_iota(jnp.int32, (1, atoms), 1)
    windows_end = 8 * BLOCK
    for block in range(GROUP_BLOCKS):
        rel = jnp.where(
            place < 384,
            block - 1 + place // BLOCK,
            jnp.where(
                place < 512,
                block - 3 + (place - 384) // HALF,
                jnp.where(
                    place < 640,
                    block + 2 + (place - 512) // HALF,
                    jnp.where(
                        place < 832,
                        block - 9 + (place - 640) // QUARTER,
                        block + 4 + (place - 832) // QUARTER,
                    ),
                ),
            ),
        )
        here = group * GROUP_BLOCKS + rel
        held = (here >= 0) & (here < total_blocks)
        late = place - windows_end
        slot_row = late % COARSE_SLOT
        coarse_block = late // COARSE_SLOT * GROUP_BLOCKS + slot_row * POOL // BLOCK
        apart = jnp.abs(coarse_block - (group * GROUP_BLOCKS + block)) > FAR_REACH
        allowed = ((place < windows_end) & held) | (
            (place >= windows_end) & (slot_row < COARSE_USED) & apart
        )
        log_size = jnp.where(
            place < 384, 0.0, jnp.where(place < 640, 1.0, jnp.where(place < windows_end, 2.0, math.log2(POOL)))
        )
        bias[pl.ds(block, 1), :] = jnp.where(allowed, log_size, -jnp.inf)

    def gather(chunk):
        for kind in (KIND_K, KIND_V):
            exchange(kind, chunk).wait_recv()

        @pl.when(inside(-outward))
        def _():
            fine_copy(chunk).start()

        pool_half(chunk, 1 - parity)
        slot = pl.ds(pl.multiple_of(group * COARSE_SLOT, COARSE_SLOT), COARSE_SLOT)
        for side in range(2):
            fours = far[chunk, side, -FAR_LOW * QUARTER : (GROUP_BLOCKS - FAR_LOW) * QUARTER]
            coarse[chunk, side, slot] = pooled(fours, COARSE_SLOT, POOL // 4)
        for way in (-1, 1):
            @pl.when(inside(way))
            def _():
                mid_copy(1, way, chunk).start()

                @pl.when(outward == way)
                def _():
                    far_copy(way, chunk).start()

        start_routes(DIRECT, chunk)

        @pl.loop(1, groups)
        def _(step):
            @pl.when(jnp.abs(lax.rem(group + step, groups) - group) > 2)
            def _():
                coarse_copy(chunk, step).start()

    def relay(chunk):
        @pl.when(inside(-outward))
        def _():
            edge_copy(0, chunk).wait_recv()
            edge_copy(1, chunk).wait_recv()

        @pl.when(inside(outward))
        def _():
            fine_copy(chunk).wait_recv()

        for way in (-1, 1):
            @pl.when(inside(-way))
            def _():
                mid_copy(0, way, chunk).wait_recv()
                mid_copy(1, way, chunk).wait_recv()
                far_copy(way, chunk).wait_recv()

        for side in range(2):
            below = pooled(fine[chunk, side, :BLOCK], HALF, 2)
            above = pooled(fine[chunk, side, 5 * BLOCK :], HALF, 2)
            mid[chunk, side, 2 * HALF : 3 * HALF] = below
            mid[chunk, side, 7 * HALF : 8 * HALF] = above
            far[chunk, side, 6 * QUARTER : 9 * QUARTER] = pooled(
                jnp.concatenate([mid[chunk, side, : 2 * HALF], below], axis=0), 3 * QUARTER, 2
            )
            far[chunk, side, 13 * QUARTER : 16 * QUARTER] = pooled(
                jnp.concatenate([above, mid[chunk, side, 8 * HALF :]], axis=0), 3 * QUARTER, 2
            )
        start_routes(SECOND_HOP, chunk)

    scale = math.log2(math.e) / math.sqrt(HEAD_DIM)

    def rows_at(ref, chunk, side, first, count, unit):
        return ref[chunk, side, pl.ds(pl.multiple_of(first * unit, unit), count * unit)]

    def attend(chunk):
        own_copy(KIND_Q, chunk).wait()
        exchange(KIND_Q, chunk).wait_recv()
        await_routes(SECOND_HOP + DIRECT, chunk)

        @pl.loop(1, groups)
        def _(step):
            giver = lax.rem(group - step + groups, groups)
            origin = pl.ds(pl.multiple_of(giver * COARSE_SLOT, COARSE_SLOT), COARSE_SLOT)

            @pl.when(jnp.abs(giver - group) > 2)
            def _():
                pltpu.make_async_remote_copy(
                    src_ref=coarse.at[chunk, :, origin], dst_ref=coarse.at[chunk, :, origin],
                    send_sem=coarse_send.at[chunk, step], recv_sem=coarse_recv.at[chunk, step],
                    device_id={"seq": partner}, device_id_type=MESH,
                ).wait_recv()

        for offset in (-2, 2):
            @pl.when(inside(offset))
            def _():
                near = pl.ds(pl.multiple_of((group + offset) * COARSE_SLOT, COARSE_SLOT), COARSE_SLOT)
                first = (offset * GROUP_BLOCKS - FAR_LOW) * QUARTER
                for side in range(2):
                    fours = far[chunk, side, first : first + GROUP_ROWS // 4]
                    coarse[chunk, side, near] = pooled(fours, COARSE_SLOT, POOL // 4)

        def attend_block(block):
            def atom_rows(side):
                return jnp.concatenate(
                    [
                        rows_at(fine, chunk, side, block, 3, BLOCK),
                        rows_at(mid, chunk, side, block, 2, HALF),
                        rows_at(mid, chunk, side, block + 5, 2, HALF),
                        rows_at(far, chunk, side, block, 6, QUARTER),
                        rows_at(far, chunk, side, block + 13, 6, QUARTER),
                        coarse[chunk, side],
                    ],
                    axis=0,
                )

            here = pl.ds(pl.multiple_of(block * BLOCK, BLOCK), BLOCK)
            scores = lax.dot_general(
                q_rows[chunk, here], atom_rows(0),
                (((1,), (1,)), ((), ())), preferred_element_type=jnp.float32,
            ) * scale + bias[pl.ds(block, 1), :]
            row_top = jnp.max(scores, axis=1, keepdims=True)
            exp_terms = jnp.exp2(scores - row_top)
            denominator = jnp.sum(exp_terms, axis=1, keepdims=True)
            weighted = jnp.dot(
                exp_terms.astype(jnp.bfloat16), atom_rows(1), preferred_element_type=jnp.float32
            )
            out_rows[chunk, here] = (weighted / denominator).astype(jnp.bfloat16)

        for block in range(half_blocks):
            attend_block((1 - parity) * half_blocks + block)
        exchange(KIND_O, chunk).start()
        for block in range(half_blocks):
            attend_block(parity * half_blocks + block)
        own_result(chunk).start()

    stages = ((gather, 0), (relay, RELAY_LAG), (attend, ATTEND_LAG))

    @pl.loop(0, chunks + ATTEND_LAG)
    def _(step):
        for stage, lag in stages:
            @pl.when((step >= lag) & (step < chunks + lag))
            def _():
                stage(step - lag)

    @pl.loop(0, chunks)
    def _(chunk):
        own_result(chunk).wait()
        exchange(KIND_O, chunk).wait_recv()
        for kind in (KIND_K, KIND_V, KIND_Q, KIND_O):
            exchange(kind, chunk).wait_send()

        @pl.when(inside(outward))
        def _():
            edge_copy(0, chunk).wait_send()
            edge_copy(1, chunk).wait_send()

        @pl.when(inside(-outward))
        def _():
            fine_copy(chunk).wait_send()

        for way in (-1, 1):
            @pl.when(inside(way))
            def _():
                mid_copy(0, way, chunk).wait_send()
                mid_copy(1, way, chunk).wait_send()
                far_copy(way, chunk).wait_send()

        for route in SECOND_HOP + DIRECT:
            @pl.when(inside(route[5]) & inside(route[5] - route[1]))
            def _():
                routed(route, chunk).wait_send()

        @pl.loop(1, groups)
        def _(step):
            @pl.when(jnp.abs(lax.rem(group + step, groups) - group) > 2)
            def _():
                coarse_copy(chunk, step).wait_send()


def per_device(queries, key_rows, value_rows):
    rows_dev, cols = queries.shape
    groups = lax.axis_size("seq") // 2
    chunks = cols // 2 // HEAD_DIM
    atoms = 8 * BLOCK + groups * COARSE_SLOT
    bf16 = jnp.bfloat16
    placed = pl.BlockSpec(memory_space=pltpu.HBM)
    return pl.pallas_call(
        functools.partial(kernel, groups),
        out_shape=jax.ShapeDtypeStruct(queries.shape, bf16),
        in_specs=[placed] * 3,
        out_specs=placed,
        scratch_shapes=[
            pltpu.VMEM((chunks, 2 * rows_dev, HEAD_DIM), bf16),
            pltpu.VMEM((chunks, 2, FINE_BLOCKS * BLOCK, HEAD_DIM), bf16),
            pltpu.VMEM((chunks, 2, MID_BLOCKS * HALF, HEAD_DIM), bf16),
            pltpu.VMEM((chunks, 2, FAR_BLOCKS * QUARTER, HEAD_DIM), bf16),
            pltpu.VMEM((chunks, 2, groups * COARSE_SLOT, HEAD_DIM), bf16),
            pltpu.VMEM((chunks, 2 * rows_dev, HEAD_DIM), bf16),
            pltpu.VMEM((8, atoms), jnp.float32),
            pltpu.SemaphoreType.DMA((chunks, KINDS)),
            pltpu.SemaphoreType.DMA((chunks, KINDS)),
            pltpu.SemaphoreType.DMA((chunks, groups)),
            pltpu.SemaphoreType.DMA((chunks, groups)),
            pltpu.SemaphoreType.DMA((chunks, 4)),
            pltpu.SemaphoreType.REGULAR((2,)),
        ],
        compiler_params=pltpu.CompilerParams(
            collective_id=0, has_side_effects=True, vmem_limit_bytes=48 * 1024 * 1024
        ),
    )(*(pltpu.with_memory_space_constraint(source, pltpu.HBM) for source in (queries, key_rows, value_rows)))


def solution(mesh):
    placed = (P("seq", "head"), P("seq", "head"), P("seq", "head"))
    return jax.shard_map(
        per_device, mesh=mesh, in_specs=placed, out_specs=P("seq", "head"), check_vma=False
    )
```

```python
import functools
import math

import jax
import jax.numpy as jnp
from jax import lax
from jax.experimental import pallas as pl
from jax.experimental.pallas import tpu as pltpu
from jax.sharding import PartitionSpec as P

HEAD_DIM = 128
BLOCK = 128
POOL = 64
MID_REACH = 3
FAR_REACH = 9

HALF = BLOCK // 2
QUARTER = BLOCK // 4
GROUP_BLOCKS = 4
GROUP_ROWS = GROUP_BLOCKS * BLOCK
COARSE_SLOT = 16
COARSE_USED = GROUP_ROWS // POOL

FINE_LOW, FINE_BLOCKS = -1, GROUP_BLOCKS + 2
MID_LOW, MID_BLOCKS = -MID_REACH, GROUP_BLOCKS + 2 * MID_REACH
FAR_LOW, FAR_BLOCKS = -FAR_REACH, GROUP_BLOCKS + 2 * FAR_REACH

KIND_K, KIND_V, KIND_Q, KIND_O, KIND_EDGE_K, KIND_EDGE_V, KIND_FINE, KIND_MID_OWN = range(8)
KIND_MID_OTHER, KIND_FAR = KIND_MID_OWN + 2, KIND_MID_OWN + 4
SECOND_HOP = (
    (13, 2, -4, 4, -8, 1),
    (14, -2, 4, 4, 8, -1),
)
DIRECT = (
    (15, 3, 3, 1, -9, 3),
    (16, -3, 0, 1, 12, -3),
)
RELAY_LAG, ATTEND_LAG = 2, 4
AHEAD, QUERY_LAG = 4, 1
STAGES = 4
KINDS = 18
KIND_LAST = 17
MESH = pl.DeviceIdType.MESH


def pool_matrix(out_rows, in_rows, group_rows):
    row = lax.broadcasted_iota(jnp.int32, (out_rows, in_rows), 0)
    col = lax.broadcasted_iota(jnp.int32, (out_rows, in_rows), 1)
    return jnp.where(col // group_rows == row, 1.0 / group_rows, 0.0).astype(jnp.bfloat16)


def pooled(source, out_rows, group_rows):
    weights = pool_matrix(out_rows, source.shape[0], group_rows)
    return jnp.dot(weights, source, preferred_element_type=jnp.float32).astype(jnp.bfloat16)


def kernel(
    groups, q_ref, k_ref, v_ref, o_ref,
    q_rows, fine, mid, far, coarse, out_rows, bias,
    stage, send, recv, coarse_send, coarse_recv, local, entered,
):
    me = lax.axis_index("seq")
    group = me // 2
    parity = me % 2
    partner = me + 1 - 2 * parity
    outward = 2 * parity - 1
    rows_dev = q_ref.shape[0]
    chunks = q_rows.shape[0]
    half_cols = chunks * HEAD_DIM
    own_first = pl.multiple_of(parity * rows_dev, rows_dev)
    other_first = pl.multiple_of((1 - parity) * rows_dev, rows_dev)
    half_blocks = GROUP_BLOCKS // 2

    def own_cols(chunk):
        return pl.ds(pl.multiple_of(parity * half_cols + chunk * HEAD_DIM, HEAD_DIM), HEAD_DIM)

    def other_cols(chunk):
        return pl.ds(pl.multiple_of((1 - parity) * half_cols + chunk * HEAD_DIM, HEAD_DIM), HEAD_DIM)

    def fine_rows(block):
        return pl.ds(pl.multiple_of((block - FINE_LOW) * BLOCK, BLOCK), BLOCK)

    def remote(src, dst, kind, chunk, target):
        return pltpu.make_async_remote_copy(
            src_ref=src, dst_ref=dst, send_sem=send.at[chunk, kind], recv_sem=recv.at[chunk, kind],
            device_id={"seq": target}, device_id_type=MESH,
        )

    def exchange(kind, chunk):
        if kind == KIND_Q:
            return remote(
                q_ref.at[:, other_cols(chunk)], q_rows.at[chunk, pl.ds(own_first, rows_dev)],
                kind, chunk, partner,
            )
        source = k_ref if kind == KIND_K else v_ref
        return remote(
            source.at[:, other_cols(chunk)], fine.at[chunk, kind, pl.ds(BLOCK + own_first, rows_dev)],
            kind, chunk, partner,
        )

    def result_copy(step, chunk):
        source = out_rows.at[chunk, pl.ds(pl.multiple_of(other_first + step * BLOCK, BLOCK), BLOCK)]
        return remote(
            source, o_ref.at[step * BLOCK : (step + 1) * BLOCK, own_cols(chunk)], KIND_O + step * (KIND_LAST - KIND_O),
            chunk, partner,
        )

    def edge_copy(side, chunk):
        source = v_ref if side else k_ref
        rows = pl.ds(pl.multiple_of(parity * (rows_dev - BLOCK), BLOCK), BLOCK)
        landing = (1 - parity) * (GROUP_BLOCKS + 1) - 1
        return remote(
            source.at[rows, own_cols(chunk)], fine.at[chunk, side, fine_rows(landing)],
            KIND_EDGE_K + side, chunk, me + 2 * outward,
        )

    def fine_copy(chunk):
        first = (1 - parity) * (GROUP_BLOCKS - 1)
        landing = parity * (GROUP_BLOCKS + 1) - 1
        return remote(
            fine.at[chunk, :, fine_rows(first)], fine.at[chunk, :, fine_rows(landing)],
            KIND_FINE, chunk, me - 2 * outward,
        )

    def mid_rows(block):
        return pl.ds(pl.multiple_of((block - MID_LOW) * HALF, HALF), HALF)

    def far_rows(first, count):
        return pl.ds((first - FAR_LOW) * QUARTER, count * QUARTER)

    def mid_copy(other, way, chunk):
        block = 2 - parity if other else 1 + parity
        return remote(
            mid.at[chunk, :, mid_rows(block)], mid.at[chunk, :, mid_rows(block - GROUP_BLOCKS * way)],
            KIND_MID_OWN + 2 * other + (way < 0), chunk, me + 2 * way,
        )

    def far_copy(way, chunk):
        first, landing = (0, -GROUP_BLOCKS) if way > 0 else (GROUP_BLOCKS - 1, 2 * GROUP_BLOCKS - 1)
        return remote(
            far.at[chunk, :, far_rows(first, 1)], far.at[chunk, :, far_rows(landing, 1)],
            KIND_FAR + (way < 0), chunk, me + 2 * way,
        )

    def routed(route, chunk):
        kind, offset, first, count, landing, hop = route
        return remote(
            far.at[chunk, :, far_rows(first, count)], far.at[chunk, :, far_rows(landing, count)],
            kind, chunk, me + 2 * hop,
        )

    def coarse_copy(chunk, step):
        target = lax.rem(group + step, groups) * 2 + parity
        slot = pl.ds(pl.multiple_of(group * COARSE_SLOT, COARSE_SLOT), COARSE_SLOT)
        return pltpu.make_async_remote_copy(
            src_ref=coarse.at[chunk, :, slot], dst_ref=coarse.at[chunk, :, slot],
            send_sem=coarse_send.at[chunk, step], recv_sem=coarse_recv.at[chunk, step],
            device_id={"seq": target}, device_id_type=MESH,
        )

    def inside(offset):
        return (group + offset >= 0) & (group + offset < groups)

    def start_routes(routes, chunk):
        for route in routes:
            @pl.when(inside(route[5]) & inside(route[5] - route[1]))
            def _():
                routed(route, chunk).start()

    def await_routes(routes, chunk):
        for route in routes:
            @pl.when(inside(-route[1]))
            def _():
                routed(route, chunk).wait_recv()

    def own_copy(kind, chunk):
        if kind == KIND_Q:
            source, target = q_ref, q_rows.at[chunk, pl.ds(own_first, rows_dev)]
        else:
            source = k_ref if kind == KIND_K else v_ref
            target = fine.at[chunk, kind, pl.ds(BLOCK + own_first, rows_dev)]
        return pltpu.make_async_copy(source.at[:, own_cols(chunk)], target, local.at[chunk, kind])

    def own_result(chunk):
        return pltpu.make_async_copy(
            out_rows.at[chunk, pl.ds(own_first, rows_dev)], o_ref.at[:, own_cols(chunk)],
            local.at[chunk, KIND_O],
        )

    @pl.loop(0, chunks)
    def _(chunk):
        coarse[chunk] = jnp.zeros(coarse.shape[1:], jnp.bfloat16)

    def start_edge(chunk):
        @pl.when(inside(outward))
        def _():
            edge_copy(0, chunk).start()
            edge_copy(1, chunk).start()

    barrier = pltpu.get_barrier_semaphore()
    pl.semaphore_signal(barrier, inc=1, device_id={"seq": partner}, device_id_type=MESH)
    for way in (1, -1):
        @pl.when(inside(way))
        def _():
            pl.semaphore_signal(barrier, inc=1, device_id={"seq": me + 2 * way}, device_id_type=MESH)

    pl.semaphore_wait(barrier, 1 + inside(1).astype(jnp.int32) + inside(-1).astype(jnp.int32))

    @pl.loop(0, chunks)
    def _(chunk):
        own_copy(KIND_K, chunk).start()
        own_copy(KIND_V, chunk).start()
        exchange(KIND_K, chunk).start()
        exchange(KIND_V, chunk).start()

        @pl.when(chunk < AHEAD)
        def _():
            start_edge(chunk)

        @pl.when(chunk >= QUERY_LAG)
        def _():
            exchange(KIND_Q, chunk - QUERY_LAG).start()

    @pl.loop(0, chunks)
    def _(chunk):
        own_copy(KIND_Q, chunk).start()

        @pl.when(chunk >= chunks - QUERY_LAG)
        def _():
            exchange(KIND_Q, chunk).start()

    def paired(slot, first, rows, stride, step):
        low = stage[slot, pl.ds(first + step, rows, stride=stride)]
        high = stage[slot, pl.ds(first + step + 1, rows, stride=stride)]
        return (0.5 * (low + high)).astype(jnp.bfloat16)

    def twos_of(slot, first, rows):
        return paired(slot, first, rows // 2, 2, 0)

    def fours_of(slot, first, rows):
        low, high = (paired(slot, first, rows // 4, 4, step).astype(jnp.float32) for step in (0, 2))
        return (0.5 * (low + high)).astype(jnp.bfloat16)

    def pool_half(chunk, half, base=0):
        first = half * rows_dev
        for side in range(2):
            rows = fine[chunk, side, pl.ds(pl.multiple_of(BLOCK + first, BLOCK), rows_dev)]
            stage[base + side] = rows.astype(jnp.float32)
        for side in range(2):
            twos = twos_of(base + side, 0, rows_dev)
            mid[chunk, side, pl.ds(pl.multiple_of(-MID_LOW * HALF + first // 2, HALF), rows_dev // 2)] = twos
            fours = fours_of(base + side, 0, rows_dev)
            far[chunk, side, pl.ds(pl.multiple_of(-FAR_LOW * QUARTER + first // 4, QUARTER), rows_dev // 4)] = fours

    def prepare(chunk):
        own_copy(KIND_K, chunk).wait()
        own_copy(KIND_V, chunk).wait()
        pool_half(chunk, parity)
        for way in (-1, 1):
            @pl.when(inside(way))
            def _():
                mid_copy(0, way, chunk).start()

                @pl.when(outward == -way)
                def _():
                    far_copy(way, chunk).start()

    @pl.loop(0, AHEAD)
    def _(chunk):
        prepare(chunk)

    for way in (1, -1):
        @pl.when(inside(-way))
        def _():
            pl.semaphore_wait(entered.at[(1 - way) // 2], 1)

        @pl.when(inside(way))
        def _():
            pl.semaphore_signal(
                entered.at[(1 - way) // 2], inc=1, device_id={"seq": me + 2 * way}, device_id_type=MESH
            )

    for window, unit, low, offset, landing, count in (
        (fine, BLOCK, FINE_LOW, 1, -1, 1),
        (fine, BLOCK, FINE_LOW, -1, 4, 1),
        (mid, HALF, MID_LOW, 1, -3, 2),
        (mid, HALF, MID_LOW, -1, 5, 2),
        (far, QUARTER, FAR_LOW, 1, -4, 1),
        (far, QUARTER, FAR_LOW, -1, 7, 1),
        (far, QUARTER, FAR_LOW, 2, -8, 4),
        (far, QUARTER, FAR_LOW, -2, 8, 4),
        (far, QUARTER, FAR_LOW, 3, -9, 1),
        (far, QUARTER, FAR_LOW, -3, 12, 1),
    ):
        @pl.when(jnp.logical_not(inside(-offset)))
        def _():
            @pl.loop(0, chunks)
            def _(chunk):
                window[chunk, :, pl.ds((landing - low) * unit, count * unit)] = jnp.zeros(
                    (2, count * unit, HEAD_DIM), jnp.bfloat16
                )

    atoms = bias.shape[1]
    total_blocks = groups * GROUP_BLOCKS
    place = lax.broadcasted_iota(jnp.int32, (1, atoms), 1)
    windows_end = 8 * BLOCK
    for block in range(GROUP_BLOCKS):
        rel = jnp.where(
            place < 384,
            block - 1 + place // BLOCK,
            jnp.where(
                place < 512,
                block - 3 + (place - 384) // HALF,
                jnp.where(
                    place < 640,
                    block + 2 + (place - 512) // HALF,
                    jnp.where(
                        place < 832,
                        block - 9 + (place - 640) // QUARTER,
                        block + 4 + (place - 832) // QUARTER,
                    ),
                ),
            ),
        )
        here = group * GROUP_BLOCKS + rel
        held = (here >= 0) & (here < total_blocks)
        late = place - windows_end
        slot_row = late % COARSE_SLOT
        slot = late // COARSE_SLOT
        giver = jnp.where(slot < 2, group + 4 * slot - 2, slot - 2)
        given = (giver >= 0) & (giver < groups) & ((slot < 2) | (jnp.abs(giver - group) > 2))
        coarse_block = giver * GROUP_BLOCKS + slot_row * POOL // BLOCK
        apart = jnp.abs(coarse_block - (group * GROUP_BLOCKS + block)) > FAR_REACH
        allowed = ((place < windows_end) & held) | (
            (place >= windows_end) & (slot_row < COARSE_USED) & given & apart
        )
        log_size = jnp.where(
            place < 384, 0.0, jnp.where(place < 640, 1.0, jnp.where(place < windows_end, 2.0, math.log2(POOL)))
        )
        bias[pl.ds(block, 1), :] = jnp.where(allowed, log_size, -jnp.inf)

    def near_coarse(chunk, side, offset):
        first = (offset * GROUP_BLOCKS - FAR_LOW) * QUARTER
        return pooled(far[chunk, side, first : first + GROUP_ROWS // 4], COARSE_SLOT, POOL // 4)

    def gather(chunk):
        for kind in (KIND_K, KIND_V):
            exchange(kind, chunk).wait_recv()

        @pl.when(inside(-outward))
        def _():
            fine_copy(chunk).start()

        pool_half(chunk, 1 - parity)
        for way in (-1, 1):
            @pl.when(inside(way))
            def _():
                mid_copy(1, way, chunk).start()

                @pl.when(outward == way)
                def _():
                    far_copy(way, chunk).start()

        start_routes(DIRECT, chunk)

        @pl.when(inside(3) | inside(-3))
        def _():
            slot = pl.ds(pl.multiple_of(group * COARSE_SLOT, COARSE_SLOT), COARSE_SLOT)
            for side in range(2):
                coarse[chunk, side, slot] = near_coarse(chunk, side, 0)

            @pl.loop(1, groups)
            def _(step):
                @pl.when(jnp.abs(lax.rem(group + step, groups) - group) > 2)
                def _():
                    coarse_copy(chunk, step).start()

    def relay(chunk):
        @pl.when(inside(-outward))
        def _():
            edge_copy(0, chunk).wait_recv()
            edge_copy(1, chunk).wait_recv()

        @pl.when(inside(outward))
        def _():
            fine_copy(chunk).wait_recv()

        for way in (-1, 1):
            @pl.when(inside(-way))
            def _():
                mid_copy(0, way, chunk).wait_recv()
                mid_copy(1, way, chunk).wait_recv()
                far_copy(way, chunk).wait_recv()

        for side in range(2):
            for end, near_mid in ((0, 0), (GROUP_BLOCKS + 1, GROUP_BLOCKS + MID_REACH + 1)):
                slot = 2 * side + (end > 0)
                stage[slot, :BLOCK] = fine[chunk, side, end * BLOCK : (end + 1) * BLOCK].astype(jnp.float32)
                stage[slot, BLOCK:] = mid[chunk, side, near_mid * HALF : (near_mid + 2) * HALF].astype(jnp.float32)
        for side in range(2):
            for end, one, two in ((0, -1, -3), (1, GROUP_BLOCKS, GROUP_BLOCKS + 1)):
                slot = 2 * side + end
                mid[chunk, side, mid_rows(one)] = twos_of(slot, 0, BLOCK)
                far[chunk, side, far_rows(one, 1)] = fours_of(slot, 0, BLOCK)
                far[chunk, side, far_rows(two, 2)] = twos_of(slot, BLOCK, BLOCK)
        start_routes(SECOND_HOP, chunk)

    scale = math.log2(math.e) / math.sqrt(HEAD_DIM)

    def rows_at(ref, chunk, side, first, count, unit):
        return ref[chunk, side, pl.ds(pl.multiple_of(first * unit, unit), count * unit)]

    def attend(chunk):
        own_copy(KIND_Q, chunk).wait()
        exchange(KIND_Q, chunk).wait_recv()
        await_routes(SECOND_HOP + DIRECT, chunk)

        @pl.when(inside(3) | inside(-3))
        def _():
            @pl.loop(1, groups)
            def _(step):
                giver = lax.rem(group - step + groups, groups)
                origin = pl.ds(pl.multiple_of(giver * COARSE_SLOT, COARSE_SLOT), COARSE_SLOT)

                @pl.when(jnp.abs(giver - group) > 2)
                def _():
                    pltpu.make_async_remote_copy(
                        src_ref=coarse.at[chunk, :, origin], dst_ref=coarse.at[chunk, :, origin],
                        send_sem=coarse_send.at[chunk, step], recv_sem=coarse_recv.at[chunk, step],
                        device_id={"seq": partner}, device_id_type=MESH,
                    ).wait_recv()

        near = [[near_coarse(chunk, side, offset) for offset in (-2, 2)] for side in range(2)]

        def atom_rows(block, side):
            return jnp.concatenate(
                [
                    rows_at(fine, chunk, side, block, 3, BLOCK),
                    rows_at(mid, chunk, side, block, 2, HALF),
                    rows_at(mid, chunk, side, block + 5, 2, HALF),
                    rows_at(far, chunk, side, block, 6, QUARTER),
                    rows_at(far, chunk, side, block + 13, 6, QUARTER),
                    *near[side],
                    coarse[chunk, side],
                ],
                axis=0,
            )

        def score_block(block):
            here = pl.ds(pl.multiple_of(block * BLOCK, BLOCK), BLOCK)
            return lax.dot_general(
                q_rows[chunk, here], atom_rows(block, 0),
                (((1,), (1,)), ((), ())), preferred_element_type=jnp.float32,
            ) * scale + bias[pl.ds(block, 1), :]

        def finish_block(block, scores):
            here = pl.ds(pl.multiple_of(block * BLOCK, BLOCK), BLOCK)
            row_top = jnp.max(scores, axis=1, keepdims=True)
            exp_terms = jnp.exp2(scores - row_top)
            denominator = jnp.sum(exp_terms, axis=1, keepdims=True)
            weighted = jnp.dot(
                exp_terms.astype(jnp.bfloat16), atom_rows(block, 1), preferred_element_type=jnp.float32
            )
            out_rows[chunk, here] = (weighted / denominator).astype(jnp.bfloat16)

        theirs = [(1 - parity) * half_blocks + step for step in range(half_blocks)]
        ours = [parity * half_blocks + step for step in range(half_blocks)]
        order = theirs + ours
        scores = score_block(order[0])
        for step in range(GROUP_BLOCKS):
            later = score_block(order[step + 1]) if step + 1 < GROUP_BLOCKS else None
            finish_block(order[step], scores)
            scores = later
            if step < half_blocks:
                result_copy(step, chunk).start()
        own_result(chunk).start()

    def look_ahead(chunk):
        @pl.when(chunk + AHEAD < chunks)
        def _():
            start_edge(chunk + AHEAD)
            prepare(chunk + AHEAD)

    stages = ((look_ahead, 0), (gather, 0), (relay, RELAY_LAG), (attend, ATTEND_LAG))

    @pl.loop(0, chunks + ATTEND_LAG)
    def _(step):
        for stage, lag in stages:
            @pl.when((step >= lag) & (step < chunks + lag))
            def _():
                stage(step - lag)

    @pl.loop(0, chunks)
    def _(chunk):
        for kind in (KIND_K, KIND_V, KIND_Q):
            exchange(kind, chunk).wait_send()

        @pl.when(inside(outward))
        def _():
            edge_copy(0, chunk).wait_send()
            edge_copy(1, chunk).wait_send()

        @pl.when(inside(-outward))
        def _():
            fine_copy(chunk).wait_send()

        for way in (-1, 1):
            @pl.when(inside(way))
            def _():
                mid_copy(0, way, chunk).wait_send()
                mid_copy(1, way, chunk).wait_send()
                far_copy(way, chunk).wait_send()

        for route in SECOND_HOP + DIRECT:
            @pl.when(inside(route[5]) & inside(route[5] - route[1]))
            def _():
                routed(route, chunk).wait_send()

        @pl.loop(1, groups)
        def _(step):
            @pl.when(jnp.abs(lax.rem(group + step, groups) - group) > 2)
            def _():
                coarse_copy(chunk, step).wait_send()

    @pl.loop(0, chunks)
    def _(chunk):
        own_result(chunk).wait()
        for step in range(half_blocks):
            result_copy(step, chunk).wait_send()
            result_copy(step, chunk).wait_recv()


def per_device(queries, key_rows, value_rows):
    rows_dev, cols = queries.shape
    groups = lax.axis_size("seq") // 2
    chunks = cols // 2 // HEAD_DIM
    atoms = 8 * BLOCK + (groups + 2) * COARSE_SLOT
    bf16 = jnp.bfloat16
    placed = pl.BlockSpec(memory_space=pltpu.HBM)
    return pl.pallas_call(
        functools.partial(kernel, groups),
        out_shape=jax.ShapeDtypeStruct(queries.shape, bf16),
        in_specs=[placed] * 3,
        out_specs=placed,
        scratch_shapes=[
            pltpu.VMEM((chunks, 2 * rows_dev, HEAD_DIM), bf16),
            pltpu.VMEM((chunks, 2, FINE_BLOCKS * BLOCK, HEAD_DIM), bf16),
            pltpu.VMEM((chunks, 2, MID_BLOCKS * HALF, HEAD_DIM), bf16),
            pltpu.VMEM((chunks, 2, FAR_BLOCKS * QUARTER, HEAD_DIM), bf16),
            pltpu.VMEM((chunks, 2, groups * COARSE_SLOT, HEAD_DIM), bf16),
            pltpu.VMEM((chunks, 2 * rows_dev, HEAD_DIM), bf16),
            pltpu.VMEM((8, atoms), jnp.float32),
            pltpu.VMEM((STAGES, rows_dev, HEAD_DIM), jnp.float32),
            pltpu.SemaphoreType.DMA((chunks, KINDS)),
            pltpu.SemaphoreType.DMA((chunks, KINDS)),
            pltpu.SemaphoreType.DMA((chunks, groups)),
            pltpu.SemaphoreType.DMA((chunks, groups)),
            pltpu.SemaphoreType.DMA((chunks, 4)),
            pltpu.SemaphoreType.REGULAR((2,)),
        ],
        compiler_params=pltpu.CompilerParams(
            collective_id=0, has_side_effects=True, vmem_limit_bytes=48 * 1024 * 1024
        ),
    )(*(pltpu.with_memory_space_constraint(source, pltpu.HBM) for source in (queries, key_rows, value_rows)))


def solution(mesh):
    placed = (P("seq", "head"), P("seq", "head"), P("seq", "head"))
    return jax.shard_map(
        per_device, mesh=mesh, in_specs=placed, out_specs=P("seq", "head"), check_vma=False
    )
```

```python
import functools
import math

import jax
import jax.numpy as jnp
from jax import lax
from jax.experimental import pallas as pl
from jax.experimental.pallas import tpu as pltpu
from jax.sharding import PartitionSpec as P

HEAD_DIM = 128
BLOCK = 128
POOL = 64
MID_REACH = 3
FAR_REACH = 9

HALF = BLOCK // 2
QUARTER = BLOCK // 4
GROUP_BLOCKS = 4
GROUP_ROWS = GROUP_BLOCKS * BLOCK
COARSE_SLOT = 16
COARSE_USED = GROUP_ROWS // POOL

FINE_LOW, FINE_BLOCKS = -1, GROUP_BLOCKS + 2
MID_LOW, MID_BLOCKS = -MID_REACH, GROUP_BLOCKS + 2 * MID_REACH
FAR_LOW, FAR_BLOCKS = -FAR_REACH, GROUP_BLOCKS + 2 * FAR_REACH

KIND_K, KIND_V, KIND_Q, KIND_O, KIND_EDGE_K, KIND_EDGE_V, KIND_FINE, KIND_MID_OWN = range(8)
KIND_MID_OTHER, KIND_FAR = KIND_MID_OWN + 2, KIND_MID_OWN + 4
SECOND_HOP = (
    (13, 2, -4, 4, -8, 1),
    (14, -2, 4, 4, 8, -1),
)
DIRECT = (
    (15, 3, 3, 1, -9, 3),
    (16, -3, 0, 1, 12, -3),
)
RELAY_LAG, ATTEND_LAG = 2, 4
AHEAD, QUERY_LAG = 5, 1
STAGES = 4
KINDS = 18
KIND_LAST = 17
MESH = pl.DeviceIdType.MESH


def pool_matrix(out_rows, in_rows, group_rows):
    row = lax.broadcasted_iota(jnp.int32, (out_rows, in_rows), 0)
    col = lax.broadcasted_iota(jnp.int32, (out_rows, in_rows), 1)
    return jnp.where(col // group_rows == row, 1.0 / group_rows, 0.0).astype(jnp.bfloat16)


def pooled(source, out_rows, group_rows):
    weights = pool_matrix(out_rows, source.shape[0], group_rows)
    return jnp.dot(weights, source, preferred_element_type=jnp.float32).astype(jnp.bfloat16)


def kernel(
    groups, q_ref, k_ref, v_ref, o_ref,
    q_rows, fine, mid, far, coarse, out_rows, bias,
    stage, send, recv, coarse_send, coarse_recv, local, entered,
):
    me = lax.axis_index("seq")
    group = me // 2
    parity = me % 2
    partner = me + 1 - 2 * parity
    outward = 2 * parity - 1
    rows_dev = q_ref.shape[0]
    chunks = q_rows.shape[0]
    half_cols = chunks * HEAD_DIM
    own_first = pl.multiple_of(parity * rows_dev, rows_dev)
    other_first = pl.multiple_of((1 - parity) * rows_dev, rows_dev)
    half_blocks = GROUP_BLOCKS // 2

    def own_cols(chunk):
        return pl.ds(pl.multiple_of(parity * half_cols + chunk * HEAD_DIM, HEAD_DIM), HEAD_DIM)

    def other_cols(chunk):
        return pl.ds(pl.multiple_of((1 - parity) * half_cols + chunk * HEAD_DIM, HEAD_DIM), HEAD_DIM)

    def fine_rows(block):
        return pl.ds(pl.multiple_of((block - FINE_LOW) * BLOCK, BLOCK), BLOCK)

    def remote(src, dst, kind, chunk, target):
        return pltpu.make_async_remote_copy(
            src_ref=src, dst_ref=dst, send_sem=send.at[chunk, kind], recv_sem=recv.at[chunk, kind],
            device_id={"seq": target}, device_id_type=MESH,
        )

    def exchange(kind, chunk):
        if kind == KIND_Q:
            return remote(
                q_ref.at[:, other_cols(chunk)], q_rows.at[chunk, pl.ds(own_first, rows_dev)],
                kind, chunk, partner,
            )
        source = k_ref if kind == KIND_K else v_ref
        return remote(
            source.at[:, other_cols(chunk)], fine.at[chunk, kind, pl.ds(BLOCK + own_first, rows_dev)],
            kind, chunk, partner,
        )

    def result_copy(step, chunk):
        source = out_rows.at[chunk, pl.ds(pl.multiple_of(other_first + step * BLOCK, BLOCK), BLOCK)]
        return remote(
            source, o_ref.at[step * BLOCK : (step + 1) * BLOCK, own_cols(chunk)], KIND_O + step * (KIND_LAST - KIND_O),
            chunk, partner,
        )

    def edge_copy(side, chunk):
        source = v_ref if side else k_ref
        rows = pl.ds(pl.multiple_of(parity * (rows_dev - BLOCK), BLOCK), BLOCK)
        landing = (1 - parity) * (GROUP_BLOCKS + 1) - 1
        return remote(
            source.at[rows, own_cols(chunk)], fine.at[chunk, side, fine_rows(landing)],
            KIND_EDGE_K + side, chunk, me + 2 * outward,
        )

    def fine_copy(chunk):
        first = (1 - parity) * (GROUP_BLOCKS - 1)
        landing = parity * (GROUP_BLOCKS + 1) - 1
        return remote(
            fine.at[chunk, :, fine_rows(first)], fine.at[chunk, :, fine_rows(landing)],
            KIND_FINE, chunk, me - 2 * outward,
        )

    def mid_rows(block):
        return pl.ds(pl.multiple_of((block - MID_LOW) * HALF, HALF), HALF)

    def far_rows(first, count):
        return pl.ds((first - FAR_LOW) * QUARTER, count * QUARTER)

    def mid_copy(other, way, chunk):
        block = 2 - parity if other else 1 + parity
        return remote(
            mid.at[chunk, :, mid_rows(block)], mid.at[chunk, :, mid_rows(block - GROUP_BLOCKS * way)],
            KIND_MID_OWN + 2 * other + (way < 0), chunk, me + 2 * way,
        )

    def far_copy(way, chunk):
        first, landing = (0, -GROUP_BLOCKS) if way > 0 else (GROUP_BLOCKS - 1, 2 * GROUP_BLOCKS - 1)
        return remote(
            far.at[chunk, :, far_rows(first, 1)], far.at[chunk, :, far_rows(landing, 1)],
            KIND_FAR + (way < 0), chunk, me + 2 * way,
        )

    def routed(route, chunk):
        kind, offset, first, count, landing, hop = route
        return remote(
            far.at[chunk, :, far_rows(first, count)], far.at[chunk, :, far_rows(landing, count)],
            kind, chunk, me + 2 * hop,
        )

    def coarse_copy(pair, step):
        target = lax.rem(group + step, groups) * 2 + parity
        slot = pl.ds(pl.multiple_of(group * COARSE_SLOT, COARSE_SLOT), COARSE_SLOT)
        return pltpu.make_async_remote_copy(
            src_ref=coarse.at[pair, :, slot], dst_ref=coarse.at[pair, :, slot],
            send_sem=coarse_send.at[pair, step], recv_sem=coarse_recv.at[pair, step],
            device_id={"seq": target}, device_id_type=MESH,
        )

    def inside(offset):
        return (group + offset >= 0) & (group + offset < groups)

    def start_routes(routes, chunk):
        for route in routes:
            @pl.when(inside(route[5]) & inside(route[5] - route[1]))
            def _():
                routed(route, chunk).start()

    def await_routes(routes, chunk):
        for route in routes:
            @pl.when(inside(-route[1]))
            def _():
                routed(route, chunk).wait_recv()

    def own_copy(kind, chunk):
        if kind == KIND_Q:
            source, target = q_ref, q_rows.at[chunk, pl.ds(own_first, rows_dev)]
        else:
            source = k_ref if kind == KIND_K else v_ref
            target = fine.at[chunk, kind, pl.ds(BLOCK + own_first, rows_dev)]
        return pltpu.make_async_copy(source.at[:, own_cols(chunk)], target, local.at[chunk, kind])

    def own_result(chunk):
        return pltpu.make_async_copy(
            out_rows.at[chunk, pl.ds(own_first, rows_dev)], o_ref.at[:, own_cols(chunk)],
            local.at[chunk, KIND_O],
        )

    @pl.loop(0, coarse.shape[0])
    def _(pair):
        coarse[pair] = jnp.zeros(coarse.shape[1:], jnp.bfloat16)

    def start_edge(chunk):
        @pl.when(inside(outward))
        def _():
            edge_copy(0, chunk).start()
            edge_copy(1, chunk).start()

    barrier = pltpu.get_barrier_semaphore()
    pl.semaphore_signal(barrier, inc=1, device_id={"seq": partner}, device_id_type=MESH)
    for way in (1, -1):
        @pl.when(inside(way))
        def _():
            pl.semaphore_signal(barrier, inc=1, device_id={"seq": me + 2 * way}, device_id_type=MESH)

    pl.semaphore_wait(barrier, 1 + inside(1).astype(jnp.int32) + inside(-1).astype(jnp.int32))

    @pl.loop(0, chunks)
    def _(chunk):
        own_copy(KIND_K, chunk).start()
        own_copy(KIND_V, chunk).start()
        exchange(KIND_K, chunk).start()
        exchange(KIND_V, chunk).start()

        @pl.when(chunk < AHEAD)
        def _():
            start_edge(chunk)

        @pl.when(chunk >= QUERY_LAG)
        def _():
            exchange(KIND_Q, chunk - QUERY_LAG).start()

    @pl.loop(0, chunks)
    def _(chunk):
        own_copy(KIND_Q, chunk).start()

        @pl.when(chunk >= chunks - QUERY_LAG)
        def _():
            exchange(KIND_Q, chunk).start()

    def paired(slot, first, rows, stride, step):
        low = stage[slot, pl.ds(first + step, rows, stride=stride)]
        high = stage[slot, pl.ds(first + step + 1, rows, stride=stride)]
        return (0.5 * (low + high)).astype(jnp.bfloat16)

    def twos_of(slot, first, rows):
        return paired(slot, first, rows // 2, 2, 0)

    def fours_of(slot, first, rows):
        low, high = (paired(slot, first, rows // 4, 4, step).astype(jnp.float32) for step in (0, 2))
        return (0.5 * (low + high)).astype(jnp.bfloat16)

    def pool_half(chunk, half, base=0):
        first = half * rows_dev
        for side in range(2):
            rows = fine[chunk, side, pl.ds(pl.multiple_of(BLOCK + first, BLOCK), rows_dev)]
            stage[base + side] = rows.astype(jnp.float32)
        for side in range(2):
            twos = twos_of(base + side, 0, rows_dev)
            mid[chunk, side, pl.ds(pl.multiple_of(-MID_LOW * HALF + first // 2, HALF), rows_dev // 2)] = twos
            fours = fours_of(base + side, 0, rows_dev)
            far[chunk, side, pl.ds(pl.multiple_of(-FAR_LOW * QUARTER + first // 4, QUARTER), rows_dev // 4)] = fours

    def prepare(chunk):
        own_copy(KIND_K, chunk).wait()
        own_copy(KIND_V, chunk).wait()
        pool_half(chunk, parity)
        for way in (-1, 1):
            @pl.when(inside(way))
            def _():
                mid_copy(0, way, chunk).start()

                @pl.when(outward == -way)
                def _():
                    far_copy(way, chunk).start()

    @pl.loop(0, AHEAD)
    def _(chunk):
        prepare(chunk)

    for way in (1, -1):
        @pl.when(inside(-way))
        def _():
            pl.semaphore_wait(entered.at[(1 - way) // 2], 1)

        @pl.when(inside(way))
        def _():
            pl.semaphore_signal(
                entered.at[(1 - way) // 2], inc=1, device_id={"seq": me + 2 * way}, device_id_type=MESH
            )

    for window, unit, low, offset, landing, count in (
        (fine, BLOCK, FINE_LOW, 1, -1, 1),
        (fine, BLOCK, FINE_LOW, -1, 4, 1),
        (mid, HALF, MID_LOW, 1, -3, 2),
        (mid, HALF, MID_LOW, -1, 5, 2),
        (far, QUARTER, FAR_LOW, 1, -4, 1),
        (far, QUARTER, FAR_LOW, -1, 7, 1),
        (far, QUARTER, FAR_LOW, 2, -8, 4),
        (far, QUARTER, FAR_LOW, -2, 8, 4),
        (far, QUARTER, FAR_LOW, 3, -9, 1),
        (far, QUARTER, FAR_LOW, -3, 12, 1),
    ):
        @pl.when(jnp.logical_not(inside(-offset)))
        def _():
            @pl.loop(0, chunks)
            def _(chunk):
                window[chunk, :, pl.ds((landing - low) * unit, count * unit)] = jnp.zeros(
                    (2, count * unit, HEAD_DIM), jnp.bfloat16
                )

    atoms = bias.shape[1]
    total_blocks = groups * GROUP_BLOCKS
    place = lax.broadcasted_iota(jnp.int32, (1, atoms), 1)
    windows_end = 8 * BLOCK
    for block in range(GROUP_BLOCKS):
        rel = jnp.where(
            place < 384,
            block - 1 + place // BLOCK,
            jnp.where(
                place < 512,
                block - 3 + (place - 384) // HALF,
                jnp.where(
                    place < 640,
                    block + 2 + (place - 512) // HALF,
                    jnp.where(
                        place < 832,
                        block - 9 + (place - 640) // QUARTER,
                        block + 4 + (place - 832) // QUARTER,
                    ),
                ),
            ),
        )
        here = group * GROUP_BLOCKS + rel
        held = (here >= 0) & (here < total_blocks)
        late = place - windows_end
        slot_row = late % COARSE_SLOT
        slot = late // COARSE_SLOT
        giver = jnp.where(slot < 2, group + 4 * slot - 2, slot - 2)
        given = (giver >= 0) & (giver < groups) & ((slot < 2) | (jnp.abs(giver - group) > 2))
        coarse_block = giver * GROUP_BLOCKS + slot_row % COARSE_USED * POOL // BLOCK
        apart = jnp.abs(coarse_block - (group * GROUP_BLOCKS + block)) > FAR_REACH
        log_size = jnp.where(
            place < 384, 0.0, jnp.where(place < 640, 1.0, jnp.where(place < windows_end, 2.0, math.log2(POOL)))
        )
        for odd in range(2):
            used = slot_row // COARSE_USED == jnp.where(slot < 2, 0, odd)
            allowed = ((place < windows_end) & held) | ((place >= windows_end) & used & given & apart)
            bias[odd * GROUP_BLOCKS + block : odd * GROUP_BLOCKS + block + 1, :] = jnp.where(
                allowed, log_size, -jnp.inf
            )

    def near_coarse(chunk, side, offset):
        first = (offset * GROUP_BLOCKS - FAR_LOW) * QUARTER
        return pooled(far[chunk, side, first : first + GROUP_ROWS // 4], COARSE_SLOT, POOL // 4)

    def gather(chunk):
        for kind in (KIND_K, KIND_V):
            exchange(kind, chunk).wait_recv()

        @pl.when(inside(-outward))
        def _():
            fine_copy(chunk).start()

        pool_half(chunk, 1 - parity)
        for way in (-1, 1):
            @pl.when(inside(way))
            def _():
                mid_copy(1, way, chunk).start()

                @pl.when(outward == way)
                def _():
                    far_copy(way, chunk).start()

        start_routes(DIRECT, chunk)

        @pl.when((inside(3) | inside(-3)) & (chunk % 2 == 1))
        def _():
            slot = pl.ds(pl.multiple_of(group * COARSE_SLOT, COARSE_SLOT), COARSE_SLOT)
            pair = chunk // 2
            own = far_rows(0, GROUP_BLOCKS)
            for side in range(2):
                fours = jnp.concatenate([far[chunk - 1, side, own], far[chunk, side, own]], axis=0)
                coarse[pair, side, slot] = pooled(fours, COARSE_SLOT, POOL // 4)

            @pl.loop(1, groups)
            def _(step):
                @pl.when(jnp.abs(lax.rem(group + step, groups) - group) > 2)
                def _():
                    coarse_copy(pair, step).start()

    def relay(chunk):
        @pl.when(inside(-outward))
        def _():
            edge_copy(0, chunk).wait_recv()
            edge_copy(1, chunk).wait_recv()

        @pl.when(inside(outward))
        def _():
            fine_copy(chunk).wait_recv()

        for way in (-1, 1):
            @pl.when(inside(-way))
            def _():
                mid_copy(0, way, chunk).wait_recv()
                mid_copy(1, way, chunk).wait_recv()
                far_copy(way, chunk).wait_recv()

        for side in range(2):
            for end, near_mid in ((0, 0), (GROUP_BLOCKS + 1, GROUP_BLOCKS + MID_REACH + 1)):
                slot = 2 * side + (end > 0)
                stage[slot, :BLOCK] = fine[chunk, side, end * BLOCK : (end + 1) * BLOCK].astype(jnp.float32)
                stage[slot, BLOCK:] = mid[chunk, side, near_mid * HALF : (near_mid + 2) * HALF].astype(jnp.float32)
        for side in range(2):
            for end, one, two in ((0, -1, -3), (1, GROUP_BLOCKS, GROUP_BLOCKS + 1)):
                slot = 2 * side + end
                mid[chunk, side, mid_rows(one)] = twos_of(slot, 0, BLOCK)
                far[chunk, side, far_rows(one, 1)] = fours_of(slot, 0, BLOCK)
                far[chunk, side, far_rows(two, 2)] = twos_of(slot, BLOCK, BLOCK)
        start_routes(SECOND_HOP, chunk)

    scale = math.log2(math.e) / math.sqrt(HEAD_DIM)

    def rows_at(ref, chunk, side, first, count, unit):
        return ref[chunk, side, pl.ds(pl.multiple_of(first * unit, unit), count * unit)]

    def attend(chunk):
        own_copy(KIND_Q, chunk).wait()
        exchange(KIND_Q, chunk).wait_recv()
        await_routes(SECOND_HOP + DIRECT, chunk)

        pair = chunk // 2

        @pl.when((inside(3) | inside(-3)) & (chunk % 2 == 0))
        def _():
            @pl.loop(1, groups)
            def _(step):
                giver = lax.rem(group - step + groups, groups)
                origin = pl.ds(pl.multiple_of(giver * COARSE_SLOT, COARSE_SLOT), COARSE_SLOT)

                @pl.when(jnp.abs(giver - group) > 2)
                def _():
                    pltpu.make_async_remote_copy(
                        src_ref=coarse.at[pair, :, origin], dst_ref=coarse.at[pair, :, origin],
                        send_sem=coarse_send.at[pair, step], recv_sem=coarse_recv.at[pair, step],
                        device_id={"seq": partner}, device_id_type=MESH,
                    ).wait_recv()

        near = [[near_coarse(chunk, side, offset) for offset in (-2, 2)] for side in range(2)]

        def atom_rows(block, side):
            return jnp.concatenate(
                [
                    rows_at(fine, chunk, side, block, 3, BLOCK),
                    rows_at(mid, chunk, side, block, 2, HALF),
                    rows_at(mid, chunk, side, block + 5, 2, HALF),
                    rows_at(far, chunk, side, block, 6, QUARTER),
                    rows_at(far, chunk, side, block + 13, 6, QUARTER),
                    *near[side],
                    coarse[pair, side],
                ],
                axis=0,
            )

        def score_block(block):
            here = pl.ds(pl.multiple_of(block * BLOCK, BLOCK), BLOCK)
            return lax.dot_general(
                q_rows[chunk, here], atom_rows(block, 0),
                (((1,), (1,)), ((), ())), preferred_element_type=jnp.float32,
            ) * scale + bias[pl.ds(chunk % 2 * GROUP_BLOCKS + block, 1), :]

        def finish_block(block, scores):
            here = pl.ds(pl.multiple_of(block * BLOCK, BLOCK), BLOCK)
            row_top = jnp.max(scores, axis=1, keepdims=True)
            exp_terms = jnp.exp2(scores - row_top)
            denominator = jnp.sum(exp_terms, axis=1, keepdims=True)
            weighted = jnp.dot(
                exp_terms.astype(jnp.bfloat16), atom_rows(block, 1), preferred_element_type=jnp.float32
            )
            out_rows[chunk, here] = (weighted / denominator).astype(jnp.bfloat16)

        theirs = [(1 - parity) * half_blocks + step for step in range(half_blocks)]
        ours = [parity * half_blocks + step for step in range(half_blocks)]
        order = theirs + ours
        scores = score_block(order[0])
        for step in range(GROUP_BLOCKS):
            later = score_block(order[step + 1]) if step + 1 < GROUP_BLOCKS else None
            finish_block(order[step], scores)
            scores = later
            if step < half_blocks:
                result_copy(step, chunk).start()
        own_result(chunk).start()

    def look_ahead(chunk):
        @pl.when(chunk + AHEAD < chunks)
        def _():
            start_edge(chunk + AHEAD)
            prepare(chunk + AHEAD)

    stages = ((look_ahead, 0), (gather, 0), (relay, RELAY_LAG), (attend, ATTEND_LAG))

    @pl.loop(0, chunks + ATTEND_LAG)
    def _(step):
        for stage, lag in stages:
            @pl.when((step >= lag) & (step < chunks + lag))
            def _():
                stage(step - lag)

    @pl.loop(0, chunks)
    def _(chunk):
        for kind in (KIND_K, KIND_V, KIND_Q):
            exchange(kind, chunk).wait_send()

        @pl.when(inside(outward))
        def _():
            edge_copy(0, chunk).wait_send()
            edge_copy(1, chunk).wait_send()

        @pl.when(inside(-outward))
        def _():
            fine_copy(chunk).wait_send()

        for way in (-1, 1):
            @pl.when(inside(way))
            def _():
                mid_copy(0, way, chunk).wait_send()
                mid_copy(1, way, chunk).wait_send()
                far_copy(way, chunk).wait_send()

        for route in SECOND_HOP + DIRECT:
            @pl.when(inside(route[5]) & inside(route[5] - route[1]))
            def _():
                routed(route, chunk).wait_send()

    @pl.loop(0, chunks // 2)
    def _(pair):
        @pl.loop(1, groups)
        def _(step):
            @pl.when(jnp.abs(lax.rem(group + step, groups) - group) > 2)
            def _():
                coarse_copy(pair, step).wait_send()

    @pl.loop(0, chunks)
    def _(chunk):
        own_result(chunk).wait()
        for step in range(half_blocks):
            result_copy(step, chunk).wait_send()
            result_copy(step, chunk).wait_recv()


def per_device(queries, key_rows, value_rows):
    rows_dev, cols = queries.shape
    groups = lax.axis_size("seq") // 2
    chunks = cols // 2 // HEAD_DIM
    atoms = 8 * BLOCK + (groups + 2) * COARSE_SLOT
    bf16 = jnp.bfloat16
    placed = pl.BlockSpec(memory_space=pltpu.HBM)
    return pl.pallas_call(
        functools.partial(kernel, groups),
        out_shape=jax.ShapeDtypeStruct(queries.shape, bf16),
        in_specs=[placed] * 3,
        out_specs=placed,
        scratch_shapes=[
            pltpu.VMEM((chunks, 2 * rows_dev, HEAD_DIM), bf16),
            pltpu.VMEM((chunks, 2, FINE_BLOCKS * BLOCK, HEAD_DIM), bf16),
            pltpu.VMEM((chunks, 2, MID_BLOCKS * HALF, HEAD_DIM), bf16),
            pltpu.VMEM((chunks, 2, FAR_BLOCKS * QUARTER, HEAD_DIM), bf16),
            pltpu.VMEM((chunks // 2, 2, groups * COARSE_SLOT, HEAD_DIM), bf16),
            pltpu.VMEM((chunks, 2 * rows_dev, HEAD_DIM), bf16),
            pltpu.VMEM((2 * GROUP_BLOCKS, atoms), jnp.float32),
            pltpu.VMEM((STAGES, rows_dev, HEAD_DIM), jnp.float32),
            pltpu.SemaphoreType.DMA((chunks, KINDS)),
            pltpu.SemaphoreType.DMA((chunks, KINDS)),
            pltpu.SemaphoreType.DMA((chunks // 2, groups)),
            pltpu.SemaphoreType.DMA((chunks // 2, groups)),
            pltpu.SemaphoreType.DMA((chunks, 4)),
            pltpu.SemaphoreType.REGULAR((2,)),
        ],
        compiler_params=pltpu.CompilerParams(
            collective_id=0, has_side_effects=True, vmem_limit_bytes=48 * 1024 * 1024
        ),
    )(*(pltpu.with_memory_space_constraint(source, pltpu.HBM) for source in (queries, key_rows, value_rows)))


def solution(mesh):
    placed = (P("seq", "head"), P("seq", "head"), P("seq", "head"))
    return jax.shard_map(
        per_device, mesh=mesh, in_specs=placed, out_specs=P("seq", "head"), check_vma=False
    )
```

```python
import functools
import math

import jax
import jax.numpy as jnp
from jax import lax
from jax.experimental import pallas as pl
from jax.experimental.pallas import tpu as pltpu
from jax.sharding import PartitionSpec as P

HEAD_DIM = 128
BLOCK = 128
POOL = 64
MID_REACH = 3
FAR_REACH = 9

HALF = BLOCK // 2
QUARTER = BLOCK // 4
GROUP_BLOCKS = 4
GROUP_ROWS = GROUP_BLOCKS * BLOCK
COARSE_SLOT = 16
COARSE_USED = GROUP_ROWS // POOL

FINE_LOW, FINE_BLOCKS = -1, GROUP_BLOCKS + 2
MID_LOW, MID_BLOCKS = -MID_REACH, GROUP_BLOCKS + 2 * MID_REACH
FAR_LOW, FAR_BLOCKS = -FAR_REACH, GROUP_BLOCKS + 2 * FAR_REACH

KIND_K, KIND_V, KIND_Q, KIND_BACK, KIND_EDGE_K, KIND_EDGE_V, KIND_FINE, KIND_MID_OWN = range(8)
KIND_MID_OTHER, KIND_FAR = KIND_MID_OWN + 2, KIND_MID_OWN + 4
SECOND_HOP = (
    (13, 2, -4, 4, -8, 1),
    (14, -2, 4, 4, 8, -1),
)
DIRECT = (
    (15, 3, 3, 1, -9, 3),
    (KIND_BACK, -3, 0, 1, 12, -3),
)
RELAY_LAG, ATTEND_LAG = 2, 4
AHEAD, QUERY_LAG = 4, 2
STAGES = 4
RECV_KINDS, KINDS = 16, 18
KIND_O, KIND_LAST = 16, 17
ALL = slice(None)
MESH = pl.DeviceIdType.MESH


def pool_matrix(out_rows, in_rows, group_rows):
    row = lax.broadcasted_iota(jnp.int32, (out_rows, in_rows), 0)
    col = lax.broadcasted_iota(jnp.int32, (out_rows, in_rows), 1)
    return jnp.where(col // group_rows == row, 1.0 / group_rows, 0.0).astype(jnp.bfloat16)


def pooled(source, out_rows, group_rows):
    weights = pool_matrix(out_rows, source.shape[0], group_rows)
    return jnp.dot(weights, source, preferred_element_type=jnp.float32).astype(jnp.bfloat16)


def kernel(
    groups, q_ref, k_ref, v_ref, o_ref,
    q_rows, fine, mid, far, coarse, out_rows, bias,
    stage, send, recv, result_recv, coarse_send, coarse_recv, local, entered,
):
    me = lax.axis_index("seq")
    group = me // 2
    parity = me % 2
    partner = me + 1 - 2 * parity
    outward = 2 * parity - 1
    rows_dev = q_ref.shape[0]
    chunks = q_rows.shape[0]
    half_cols = chunks * HEAD_DIM
    own_first = pl.multiple_of(parity * rows_dev, rows_dev)
    other_first = pl.multiple_of((1 - parity) * rows_dev, rows_dev)
    half_blocks = GROUP_BLOCKS // 2

    def own_cols(chunk):
        if chunk is ALL:
            return pl.ds(pl.multiple_of(parity * half_cols, HEAD_DIM), half_cols)
        return pl.ds(pl.multiple_of(parity * half_cols + chunk * HEAD_DIM, HEAD_DIM), HEAD_DIM)

    def other_cols(chunk):
        if chunk is ALL:
            return pl.ds(pl.multiple_of((1 - parity) * half_cols, HEAD_DIM), half_cols)
        return pl.ds(pl.multiple_of((1 - parity) * half_cols + chunk * HEAD_DIM, HEAD_DIM), HEAD_DIM)

    def fine_rows(block):
        return pl.ds(pl.multiple_of((block - FINE_LOW) * BLOCK, BLOCK), BLOCK)

    def remote(src, dst, kind, chunk, target):
        if kind in (KIND_O, KIND_LAST):
            arrived = result_recv.at[kind - KIND_O]
        else:
            arrived = recv.at[0 if chunk is ALL else chunk, kind]
        return pltpu.make_async_remote_copy(
            src_ref=src, dst_ref=dst, send_sem=send.at[kind], recv_sem=arrived,
            device_id={"seq": target}, device_id_type=MESH,
        )

    def exchange(kind, chunk):
        if kind == KIND_Q:
            return remote(
                q_ref.at[:, other_cols(chunk)], q_rows.at[chunk, pl.ds(own_first, rows_dev)],
                kind, chunk, partner,
            )
        source = k_ref if kind == KIND_K else v_ref
        return remote(
            source.at[:, other_cols(chunk)], fine.at[chunk, kind, pl.ds(BLOCK + own_first, rows_dev)],
            kind, chunk, partner,
        )

    def result_copy(step, chunk):
        source = out_rows.at[chunk, pl.ds(pl.multiple_of(other_first + step * BLOCK, BLOCK), BLOCK)]
        return remote(
            source, o_ref.at[step * BLOCK : (step + 1) * BLOCK, own_cols(chunk)], KIND_O + step * (KIND_LAST - KIND_O),
            chunk, partner,
        )

    def edge_copy(side, chunk):
        source = v_ref if side else k_ref
        rows = pl.ds(pl.multiple_of(parity * (rows_dev - BLOCK), BLOCK), BLOCK)
        landing = (1 - parity) * (GROUP_BLOCKS + 1) - 1
        return remote(
            source.at[rows, own_cols(chunk)], fine.at[chunk, side, fine_rows(landing)],
            KIND_EDGE_K + side, chunk, me + 2 * outward,
        )

    def fine_copy(chunk):
        first = (1 - parity) * (GROUP_BLOCKS - 1)
        landing = parity * (GROUP_BLOCKS + 1) - 1
        return remote(
            fine.at[chunk, :, fine_rows(first)], fine.at[chunk, :, fine_rows(landing)],
            KIND_FINE, chunk, me - 2 * outward,
        )

    def mid_rows(block):
        return pl.ds(pl.multiple_of((block - MID_LOW) * HALF, HALF), HALF)

    def far_rows(first, count):
        return pl.ds((first - FAR_LOW) * QUARTER, count * QUARTER)

    def mid_copy(other, way, chunk):
        block = 2 - parity if other else 1 + parity
        return remote(
            mid.at[chunk, :, mid_rows(block)], mid.at[chunk, :, mid_rows(block - GROUP_BLOCKS * way)],
            KIND_MID_OWN + 2 * other + (way < 0), chunk, me + 2 * way,
        )

    def far_copy(way, chunk):
        first, landing = (0, -GROUP_BLOCKS) if way > 0 else (GROUP_BLOCKS - 1, 2 * GROUP_BLOCKS - 1)
        return remote(
            far.at[chunk, :, far_rows(first, 1)], far.at[chunk, :, far_rows(landing, 1)],
            KIND_FAR + (way < 0), chunk, me + 2 * way,
        )

    def routed(route, chunk):
        kind, offset, first, count, landing, hop = route
        return remote(
            far.at[chunk, :, far_rows(first, count)], far.at[chunk, :, far_rows(landing, count)],
            kind, chunk, me + 2 * hop,
        )

    def coarse_copy(pair, step):
        target = lax.rem(group + step, groups) * 2 + parity
        slot = pl.ds(pl.multiple_of(group * COARSE_SLOT, COARSE_SLOT), COARSE_SLOT)
        return pltpu.make_async_remote_copy(
            src_ref=coarse.at[pair, :, slot], dst_ref=coarse.at[pair, :, slot],
            send_sem=coarse_send.at[pair, step], recv_sem=coarse_recv.at[pair, step],
            device_id={"seq": target}, device_id_type=MESH,
        )

    def inside(offset):
        return (group + offset >= 0) & (group + offset < groups)

    def start_routes(routes, chunk):
        for route in routes:
            @pl.when(inside(route[5]) & inside(route[5] - route[1]))
            def _():
                routed(route, chunk).start()

    def await_routes(routes, chunk):
        for route in routes:
            @pl.when(inside(-route[1]))
            def _():
                routed(route, chunk).wait_recv()

    def own_copy(kind, chunk):
        if kind == KIND_Q:
            source, target = q_ref, q_rows.at[chunk, pl.ds(own_first, rows_dev)]
        else:
            source = k_ref if kind == KIND_K else v_ref
            target = fine.at[chunk, kind, pl.ds(BLOCK + own_first, rows_dev)]
        return pltpu.make_async_copy(source.at[:, own_cols(chunk)], target, local.at[chunk, kind])

    def own_result(chunk):
        return pltpu.make_async_copy(
            out_rows.at[chunk, pl.ds(own_first, rows_dev)], o_ref.at[:, own_cols(chunk)], local.at[0, 3],
        )

    def start_edge(chunk):
        @pl.when(inside(outward))
        def _():
            edge_copy(0, chunk).start()
            edge_copy(1, chunk).start()

    barrier = pltpu.get_barrier_semaphore()
    pl.semaphore_signal(barrier, inc=1, device_id={"seq": partner}, device_id_type=MESH)
    for way in (1, -1):
        @pl.when(inside(way))
        def _():
            pl.semaphore_signal(barrier, inc=1, device_id={"seq": me + 2 * way}, device_id_type=MESH)

    @pl.loop(0, coarse.shape[0])
    def _(pair):
        coarse[pair] = jnp.zeros(coarse.shape[1:], jnp.bfloat16)

    pl.semaphore_wait(barrier, 1 + inside(1).astype(jnp.int32) + inside(-1).astype(jnp.int32))

    @pl.loop(0, chunks)
    def _(chunk):
        own_copy(KIND_K, chunk).start()
        own_copy(KIND_V, chunk).start()
        exchange(KIND_K, chunk).start()
        exchange(KIND_V, chunk).start()

        @pl.when(chunk < AHEAD)
        def _():
            start_edge(chunk)

        @pl.when(chunk >= QUERY_LAG)
        def _():
            exchange(KIND_Q, chunk - QUERY_LAG).start()

    @pl.loop(0, chunks)
    def _(chunk):
        own_copy(KIND_Q, chunk).start()

        @pl.when(chunk >= chunks - QUERY_LAG)
        def _():
            exchange(KIND_Q, chunk).start()

    def paired(slot, first, rows, stride, step):
        low = stage[slot, pl.ds(first + step, rows, stride=stride)]
        high = stage[slot, pl.ds(first + step + 1, rows, stride=stride)]
        return (0.5 * (low + high)).astype(jnp.bfloat16)

    def twos_of(slot, first, rows):
        return paired(slot, first, rows // 2, 2, 0)

    def fours_of(slot, first, rows):
        low, high = (paired(slot, first, rows // 4, 4, step).astype(jnp.float32) for step in (0, 2))
        return (0.5 * (low + high)).astype(jnp.bfloat16)

    def pool_half(chunk, half, base=0):
        first = half * rows_dev
        for side in range(2):
            rows = fine[chunk, side, pl.ds(pl.multiple_of(BLOCK + first, BLOCK), rows_dev)]
            stage[base + side] = rows.astype(jnp.float32)
        for side in range(2):
            twos = twos_of(base + side, 0, rows_dev)
            mid[chunk, side, pl.ds(pl.multiple_of(-MID_LOW * HALF + first // 2, HALF), rows_dev // 2)] = twos
            fours = fours_of(base + side, 0, rows_dev)
            far[chunk, side, pl.ds(pl.multiple_of(-FAR_LOW * QUARTER + first // 4, QUARTER), rows_dev // 4)] = fours

    def prepare(chunk):
        own_copy(KIND_K, chunk).wait()
        own_copy(KIND_V, chunk).wait()
        pool_half(chunk, parity)
        for way in (-1, 1):
            @pl.when(inside(way))
            def _():
                mid_copy(0, way, chunk).start()

                @pl.when(outward == -way)
                def _():
                    far_copy(way, chunk).start()

    @pl.loop(0, AHEAD)
    def _(chunk):
        prepare(chunk)

    for way in (1, -1):
        @pl.when(inside(-way))
        def _():
            pl.semaphore_wait(entered.at[(1 - way) // 2], 1)

        @pl.when(inside(way))
        def _():
            pl.semaphore_signal(
                entered.at[(1 - way) // 2], inc=1, device_id={"seq": me + 2 * way}, device_id_type=MESH
            )

    for window, unit, low, offset, landing, count in (
        (fine, BLOCK, FINE_LOW, 1, -1, 1),
        (fine, BLOCK, FINE_LOW, -1, 4, 1),
        (mid, HALF, MID_LOW, 1, -3, 2),
        (mid, HALF, MID_LOW, -1, 5, 2),
        (far, QUARTER, FAR_LOW, 1, -4, 1),
        (far, QUARTER, FAR_LOW, -1, 7, 1),
        (far, QUARTER, FAR_LOW, 2, -8, 4),
        (far, QUARTER, FAR_LOW, -2, 8, 4),
        (far, QUARTER, FAR_LOW, 3, -9, 1),
        (far, QUARTER, FAR_LOW, -3, 12, 1),
    ):
        @pl.when(jnp.logical_not(inside(-offset)))
        def _():
            @pl.loop(0, chunks)
            def _(chunk):
                window[chunk, :, pl.ds((landing - low) * unit, count * unit)] = jnp.zeros(
                    (2, count * unit, HEAD_DIM), jnp.bfloat16
                )

    atoms = bias.shape[1]
    total_blocks = groups * GROUP_BLOCKS
    place = lax.broadcasted_iota(jnp.int32, (1, atoms), 1)
    windows_end = 8 * BLOCK
    for block in range(GROUP_BLOCKS):
        rel = jnp.where(
            place < 384,
            block - 1 + place // BLOCK,
            jnp.where(
                place < 512,
                block - 3 + (place - 384) // HALF,
                jnp.where(
                    place < 640,
                    block + 2 + (place - 512) // HALF,
                    jnp.where(
                        place < 832,
                        block - 9 + (place - 640) // QUARTER,
                        block + 4 + (place - 832) // QUARTER,
                    ),
                ),
            ),
        )
        here = group * GROUP_BLOCKS + rel
        held = (here >= 0) & (here < total_blocks)
        late = place - windows_end
        slot_row = late % COARSE_SLOT
        slot = late // COARSE_SLOT
        giver = jnp.where(slot < 2, group + 4 * slot - 2, slot - 2)
        given = (giver >= 0) & (giver < groups) & ((slot < 2) | (jnp.abs(giver - group) > 2))
        coarse_block = giver * GROUP_BLOCKS + slot_row % COARSE_USED * POOL // BLOCK
        apart = jnp.abs(coarse_block - (group * GROUP_BLOCKS + block)) > FAR_REACH
        log_size = jnp.where(
            place < 384, 0.0, jnp.where(place < 640, 1.0, jnp.where(place < windows_end, 2.0, math.log2(POOL)))
        )
        for odd in range(2):
            used = slot_row // COARSE_USED == jnp.where(slot < 2, 0, odd)
            allowed = ((place < windows_end) & held) | ((place >= windows_end) & used & given & apart)
            bias[odd * GROUP_BLOCKS + block : odd * GROUP_BLOCKS + block + 1, :] = jnp.where(
                allowed, log_size, -jnp.inf
            )

    def near_coarse(chunk, side, offset):
        first = (offset * GROUP_BLOCKS - FAR_LOW) * QUARTER
        return pooled(far[chunk, side, first : first + GROUP_ROWS // 4], COARSE_SLOT, POOL // 4)

    def gather(chunk):
        for kind in (KIND_K, KIND_V):
            exchange(kind, chunk).wait_recv()

        @pl.when(inside(-outward))
        def _():
            fine_copy(chunk).start()

        pool_half(chunk, 1 - parity)
        for way in (-1, 1):
            @pl.when(inside(way))
            def _():
                mid_copy(1, way, chunk).start()

                @pl.when(outward == way)
                def _():
                    far_copy(way, chunk).start()

        start_routes(DIRECT, chunk)

        @pl.when((inside(3) | inside(-3)) & (chunk % 2 == 1))
        def _():
            slot = pl.ds(pl.multiple_of(group * COARSE_SLOT, COARSE_SLOT), COARSE_SLOT)
            pair = chunk // 2
            own = far_rows(0, GROUP_BLOCKS)
            for side in range(2):
                fours = jnp.concatenate([far[chunk - 1, side, own], far[chunk, side, own]], axis=0)
                coarse[pair, side, slot] = pooled(fours, COARSE_SLOT, POOL // 4)

            @pl.loop(1, groups)
            def _(step):
                @pl.when(jnp.abs(lax.rem(group + step, groups) - group) > 2)
                def _():
                    coarse_copy(pair, step).start()

    def relay(chunk):
        @pl.when(inside(-outward))
        def _():
            edge_copy(0, chunk).wait_recv()
            edge_copy(1, chunk).wait_recv()

        @pl.when(inside(outward))
        def _():
            fine_copy(chunk).wait_recv()

        for way in (-1, 1):
            @pl.when(inside(-way))
            def _():
                mid_copy(0, way, chunk).wait_recv()
                mid_copy(1, way, chunk).wait_recv()
                far_copy(way, chunk).wait_recv()

        for side in range(2):
            for end, near_mid in ((0, 0), (GROUP_BLOCKS + 1, GROUP_BLOCKS + MID_REACH + 1)):
                slot = 2 * side + (end > 0)
                stage[slot, :BLOCK] = fine[chunk, side, end * BLOCK : (end + 1) * BLOCK].astype(jnp.float32)
                stage[slot, BLOCK:] = mid[chunk, side, near_mid * HALF : (near_mid + 2) * HALF].astype(jnp.float32)
        for side in range(2):
            for end, one, two in ((0, -1, -3), (1, GROUP_BLOCKS, GROUP_BLOCKS + 1)):
                slot = 2 * side + end
                mid[chunk, side, mid_rows(one)] = twos_of(slot, 0, BLOCK)
                far[chunk, side, far_rows(one, 1)] = fours_of(slot, 0, BLOCK)
                far[chunk, side, far_rows(two, 2)] = twos_of(slot, BLOCK, BLOCK)
        start_routes(SECOND_HOP, chunk)

    scale = math.log2(math.e) / math.sqrt(HEAD_DIM)

    def rows_at(ref, chunk, side, first, count, unit):
        return ref[chunk, side, pl.ds(pl.multiple_of(first * unit, unit), count * unit)]

    def attend(chunk):
        own_copy(KIND_Q, chunk).wait()
        exchange(KIND_Q, chunk).wait_recv()
        await_routes(SECOND_HOP + DIRECT, chunk)

        pair = chunk // 2

        @pl.when((inside(3) | inside(-3)) & (chunk % 2 == 0))
        def _():
            @pl.loop(1, groups)
            def _(step):
                giver = lax.rem(group - step + groups, groups)
                origin = pl.ds(pl.multiple_of(giver * COARSE_SLOT, COARSE_SLOT), COARSE_SLOT)

                @pl.when(jnp.abs(giver - group) > 2)
                def _():
                    pltpu.make_async_remote_copy(
                        src_ref=coarse.at[pair, :, origin], dst_ref=coarse.at[pair, :, origin],
                        send_sem=coarse_send.at[pair, step], recv_sem=coarse_recv.at[pair, step],
                        device_id={"seq": partner}, device_id_type=MESH,
                    ).wait_recv()

        near = [[near_coarse(chunk, side, offset) for offset in (-2, 2)] for side in range(2)]

        def atom_rows(block, side):
            return jnp.concatenate(
                [
                    rows_at(fine, chunk, side, block, 3, BLOCK),
                    rows_at(mid, chunk, side, block, 2, HALF),
                    rows_at(mid, chunk, side, block + 5, 2, HALF),
                    rows_at(far, chunk, side, block, 6, QUARTER),
                    rows_at(far, chunk, side, block + 13, 6, QUARTER),
                    *near[side],
                    coarse[pair, side],
                ],
                axis=0,
            )

        def score_block(block):
            here = pl.ds(pl.multiple_of(block * BLOCK, BLOCK), BLOCK)
            return lax.dot_general(
                q_rows[chunk, here], atom_rows(block, 0),
                (((1,), (1,)), ((), ())), preferred_element_type=jnp.float32,
            ) * scale + bias[pl.ds(chunk % 2 * GROUP_BLOCKS + block, 1), :]

        def finish_block(block, scores):
            here = pl.ds(pl.multiple_of(block * BLOCK, BLOCK), BLOCK)
            row_top = jnp.max(scores, axis=1, keepdims=True)
            exp_terms = jnp.exp2(scores - row_top)
            denominator = jnp.sum(exp_terms, axis=1, keepdims=True)
            weighted = jnp.dot(
                exp_terms.astype(jnp.bfloat16), atom_rows(block, 1), preferred_element_type=jnp.float32
            )
            out_rows[chunk, here] = (weighted / denominator).astype(jnp.bfloat16)

        theirs = [(1 - parity) * half_blocks + step for step in range(half_blocks)]
        ours = [parity * half_blocks + step for step in range(half_blocks)]
        order = theirs + ours
        scores = [score_block(order[0]), score_block(order[1])]
        for step in range(GROUP_BLOCKS):
            if step + 2 < GROUP_BLOCKS:
                scores.append(score_block(order[step + 2]))
            finish_block(order[step], scores[step])
            if step < half_blocks:
                result_copy(step, chunk).start()
        own_result(chunk).start()

    def look_ahead(chunk):
        @pl.when(chunk + AHEAD < chunks)
        def _():
            start_edge(chunk + AHEAD)
            prepare(chunk + AHEAD)

    stages = ((gather, 0), (look_ahead, 0), (relay, RELAY_LAG), (attend, ATTEND_LAG))

    @pl.loop(0, chunks + ATTEND_LAG)
    def _(step):
        for stage, lag in stages:
            @pl.when((step >= lag) & (step < chunks + lag))
            def _():
                stage(step - lag)

    for kind in (KIND_K, KIND_V, KIND_Q):
        exchange(kind, ALL).wait_send()

    @pl.when(inside(outward))
    def _():
        edge_copy(0, ALL).wait_send()
        edge_copy(1, ALL).wait_send()

    @pl.when(inside(-outward))
    def _():
        fine_copy(ALL).wait_send()

    for way in (-1, 1):
        @pl.when(inside(way))
        def _():
            mid_copy(0, way, ALL).wait_send()
            mid_copy(1, way, ALL).wait_send()
            far_copy(way, ALL).wait_send()

    for route in SECOND_HOP + DIRECT:
        @pl.when(inside(route[5]) & inside(route[5] - route[1]))
        def _():
            routed(route, ALL).wait_send()

    @pl.loop(0, chunks // 2)
    def _(pair):
        @pl.loop(1, groups)
        def _(step):
            @pl.when(jnp.abs(lax.rem(group + step, groups) - group) > 2)
            def _():
                coarse_copy(pair, step).wait_send()

    whole = q_rows.at[:, pl.ds(own_first, rows_dev)]
    pltpu.make_async_copy(whole, whole, local.at[0, 3]).wait()
    for step in range(half_blocks):
        result_copy(step, ALL).wait_send()
        result_copy(step, ALL).wait_recv()


def per_device(queries, key_rows, value_rows):
    rows_dev, cols = queries.shape
    groups = lax.axis_size("seq") // 2
    chunks = cols // 2 // HEAD_DIM
    atoms = 8 * BLOCK + (groups + 2) * COARSE_SLOT
    bf16 = jnp.bfloat16
    placed = pl.BlockSpec(memory_space=pltpu.HBM)
    return pl.pallas_call(
        functools.partial(kernel, groups),
        out_shape=jax.ShapeDtypeStruct(queries.shape, bf16),
        in_specs=[placed] * 3,
        out_specs=placed,
        scratch_shapes=[
            pltpu.VMEM((chunks, 2 * rows_dev, HEAD_DIM), bf16),
            pltpu.VMEM((chunks, 2, FINE_BLOCKS * BLOCK, HEAD_DIM), bf16),
            pltpu.VMEM((chunks, 2, MID_BLOCKS * HALF, HEAD_DIM), bf16),
            pltpu.VMEM((chunks, 2, FAR_BLOCKS * QUARTER, HEAD_DIM), bf16),
            pltpu.VMEM((chunks // 2, 2, groups * COARSE_SLOT, HEAD_DIM), bf16),
            pltpu.VMEM((chunks, 2 * rows_dev, HEAD_DIM), bf16),
            pltpu.VMEM((2 * GROUP_BLOCKS, atoms), jnp.float32),
            pltpu.VMEM((STAGES, rows_dev, HEAD_DIM), jnp.float32),
            pltpu.SemaphoreType.DMA((KINDS,)),
            pltpu.SemaphoreType.DMA((chunks, RECV_KINDS)),
            pltpu.SemaphoreType.DMA((2,)),
            pltpu.SemaphoreType.DMA((chunks // 2, groups)),
            pltpu.SemaphoreType.DMA((chunks // 2, groups)),
            pltpu.SemaphoreType.DMA((chunks, 4)),
            pltpu.SemaphoreType.REGULAR((2,)),
        ],
        compiler_params=pltpu.CompilerParams(
            collective_id=0, has_side_effects=True, vmem_limit_bytes=48 * 1024 * 1024
        ),
    )(*(pltpu.with_memory_space_constraint(source, pltpu.HBM) for source in (queries, key_rows, value_rows)))


def solution(mesh):
    placed = (P("seq", "head"), P("seq", "head"), P("seq", "head"))
    return jax.shard_map(
        per_device, mesh=mesh, in_specs=placed, out_specs=P("seq", "head"), check_vma=False
    )
```

```python
import functools
import math

import jax
import jax.numpy as jnp
from jax import lax
from jax.experimental import pallas as pl
from jax.experimental.pallas import tpu as pltpu
from jax.sharding import PartitionSpec as P

HEAD_DIM = 128
BLOCK = 128
POOL = 64
MID_REACH = 3
FAR_REACH = 9

HALF = BLOCK // 2
QUARTER = BLOCK // 4
GROUP_BLOCKS = 4
GROUP_ROWS = GROUP_BLOCKS * BLOCK
COARSE_SLOT = 16
COARSE_USED = GROUP_ROWS // POOL

FINE_LOW, FINE_BLOCKS = -1, GROUP_BLOCKS + 2
MID_LOW, MID_BLOCKS = -MID_REACH, GROUP_BLOCKS + 2 * MID_REACH
FAR_LOW, FAR_BLOCKS = -FAR_REACH, GROUP_BLOCKS + 2 * FAR_REACH

KIND_K, KIND_V, KIND_Q, KIND_BACK, KIND_EDGE_K, KIND_EDGE_V, KIND_FINE, KIND_MID_OWN = range(8)
KIND_MID_OTHER, KIND_FAR = KIND_MID_OWN + 2, KIND_MID_OWN + 4
SECOND_HOP = (
    (13, 2, -4, 4, -8, 1),
    (14, -2, 4, 4, 8, -1),
)
DIRECT = (
    (15, 3, 3, 1, -9, 3),
    (KIND_BACK, -3, 0, 1, 12, -3),
)
RELAY_LAG, ATTEND_LAG = 2, 4
AHEAD, QUERY_LAG = 4, 2
STAGES = 4
RECV_OF = (0, 0, 1, 2, 3, 3, 4, 5, 6, 5, 6, 5, 6, 7, 8, 9)
RECV_KINDS, KINDS = 10, 18
KIND_O, KIND_LAST = 16, 17
ALL = slice(None)
MESH = pl.DeviceIdType.MESH


def pool_matrix(out_rows, in_rows, group_rows):
    row = lax.broadcasted_iota(jnp.int32, (out_rows, in_rows), 0)
    col = lax.broadcasted_iota(jnp.int32, (out_rows, in_rows), 1)
    return jnp.where(col // group_rows == row, 1.0 / group_rows, 0.0).astype(jnp.bfloat16)


def pooled(source, out_rows, group_rows):
    weights = pool_matrix(out_rows, source.shape[0], group_rows)
    return jnp.dot(weights, source, preferred_element_type=jnp.float32).astype(jnp.bfloat16)


def kernel(
    groups, q_ref, k_ref, v_ref, o_ref,
    q_rows, fine, mid, far, coarse, out_rows, bias,
    stage, send, recv, result_recv, coarse_send, coarse_recv, local, entered,
):
    me = lax.axis_index("seq")
    group = me // 2
    parity = me % 2
    partner = me + 1 - 2 * parity
    outward = 2 * parity - 1
    rows_dev = q_ref.shape[0]
    chunks = q_rows.shape[0]
    half_cols = chunks * HEAD_DIM
    own_first = pl.multiple_of(parity * rows_dev, rows_dev)
    other_first = pl.multiple_of((1 - parity) * rows_dev, rows_dev)
    half_blocks = GROUP_BLOCKS // 2

    def own_cols(chunk):
        if chunk is ALL:
            return pl.ds(pl.multiple_of(parity * half_cols, HEAD_DIM), half_cols)
        return pl.ds(pl.multiple_of(parity * half_cols + chunk * HEAD_DIM, HEAD_DIM), HEAD_DIM)

    def other_cols(chunk):
        if chunk is ALL:
            return pl.ds(pl.multiple_of((1 - parity) * half_cols, HEAD_DIM), half_cols)
        return pl.ds(pl.multiple_of((1 - parity) * half_cols + chunk * HEAD_DIM, HEAD_DIM), HEAD_DIM)

    def fine_rows(block):
        return pl.ds(pl.multiple_of((block - FINE_LOW) * BLOCK, BLOCK), BLOCK)

    def remote(src, dst, kind, chunk, target):
        if kind in (KIND_O, KIND_LAST):
            arrived = result_recv.at[kind - KIND_O]
        else:
            arrived = recv.at[0 if chunk is ALL else chunk, RECV_OF[kind]]
        return pltpu.make_async_remote_copy(
            src_ref=src, dst_ref=dst, send_sem=send.at[kind], recv_sem=arrived,
            device_id={"seq": target}, device_id_type=MESH,
        )

    def exchange(kind, chunk):
        if kind == KIND_Q:
            return remote(
                q_ref.at[:, other_cols(chunk)], q_rows.at[chunk, pl.ds(own_first, rows_dev)],
                kind, chunk, partner,
            )
        source = k_ref if kind == KIND_K else v_ref
        return remote(
            source.at[:, other_cols(chunk)], fine.at[chunk, kind, pl.ds(BLOCK + own_first, rows_dev)],
            kind, chunk, partner,
        )

    def result_copy(step, chunk):
        source = out_rows.at[chunk, pl.ds(pl.multiple_of(other_first + step * BLOCK, BLOCK), BLOCK)]
        return remote(
            source, o_ref.at[step * BLOCK : (step + 1) * BLOCK, own_cols(chunk)], KIND_O + step * (KIND_LAST - KIND_O),
            chunk, partner,
        )

    def edge_copy(side, chunk):
        source = v_ref if side else k_ref
        rows = pl.ds(pl.multiple_of(parity * (rows_dev - BLOCK), BLOCK), BLOCK)
        landing = (1 - parity) * (GROUP_BLOCKS + 1) - 1
        return remote(
            source.at[rows, own_cols(chunk)], fine.at[chunk, side, fine_rows(landing)],
            KIND_EDGE_K + side, chunk, me + 2 * outward,
        )

    def fine_copy(chunk):
        first = (1 - parity) * (GROUP_BLOCKS - 1)
        landing = parity * (GROUP_BLOCKS + 1) - 1
        return remote(
            fine.at[chunk, :, fine_rows(first)], fine.at[chunk, :, fine_rows(landing)],
            KIND_FINE, chunk, me - 2 * outward,
        )

    def mid_rows(block):
        return pl.ds(pl.multiple_of((block - MID_LOW) * HALF, HALF), HALF)

    def far_rows(first, count):
        return pl.ds((first - FAR_LOW) * QUARTER, count * QUARTER)

    def mid_copy(other, way, chunk):
        block = 2 - parity if other else 1 + parity
        return remote(
            mid.at[chunk, :, mid_rows(block)], mid.at[chunk, :, mid_rows(block - GROUP_BLOCKS * way)],
            KIND_MID_OWN + 2 * other + (way < 0), chunk, me + 2 * way,
        )

    def far_copy(way, chunk):
        first, landing = (0, -GROUP_BLOCKS) if way > 0 else (GROUP_BLOCKS - 1, 2 * GROUP_BLOCKS - 1)
        return remote(
            far.at[chunk, :, far_rows(first, 1)], far.at[chunk, :, far_rows(landing, 1)],
            KIND_FAR + (way < 0), chunk, me + 2 * way,
        )

    def routed(route, chunk):
        kind, offset, first, count, landing, hop = route
        return remote(
            far.at[chunk, :, far_rows(first, count)], far.at[chunk, :, far_rows(landing, count)],
            kind, chunk, me + 2 * hop,
        )

    def coarse_copy(pair, step):
        target = lax.rem(group + step, groups) * 2 + parity
        slot = pl.ds(pl.multiple_of(group * COARSE_SLOT, COARSE_SLOT), COARSE_SLOT)
        return pltpu.make_async_remote_copy(
            src_ref=coarse.at[pair, :, slot], dst_ref=coarse.at[pair, :, slot],
            send_sem=coarse_send.at[pair, step], recv_sem=coarse_recv.at[pair, step],
            device_id={"seq": target}, device_id_type=MESH,
        )

    def await_bytes(ref, semaphore):
        pltpu.make_async_copy(ref, ref, semaphore).wait()

    def inside(offset):
        return (group + offset >= 0) & (group + offset < groups)

    def start_routes(routes, chunk):
        for route in routes:
            @pl.when(inside(route[5]) & inside(route[5] - route[1]))
            def _():
                routed(route, chunk).start()

    def await_routes(routes, chunk):
        for route in routes:
            @pl.when(inside(-route[1]))
            def _():
                routed(route, chunk).wait_recv()

    def own_copy(kind, chunk):
        if kind == KIND_Q:
            source, target = q_ref, q_rows.at[chunk, pl.ds(own_first, rows_dev)]
        else:
            source = k_ref if kind == KIND_K else v_ref
            target = fine.at[chunk, kind, pl.ds(BLOCK + own_first, rows_dev)]
        return pltpu.make_async_copy(source.at[:, own_cols(chunk)], target, local.at[chunk, kind // 2])

    def own_result(chunk):
        return pltpu.make_async_copy(
            out_rows.at[chunk, pl.ds(own_first, rows_dev)], o_ref.at[:, own_cols(chunk)], result_recv.at[2],
        )

    def start_edge(chunk):
        @pl.when(inside(outward))
        def _():
            edge_copy(0, chunk).start()
            edge_copy(1, chunk).start()

    barrier = pltpu.get_barrier_semaphore()
    pl.semaphore_signal(barrier, inc=1, device_id={"seq": partner}, device_id_type=MESH)
    for way in (1, -1):
        @pl.when(inside(way))
        def _():
            pl.semaphore_signal(barrier, inc=1, device_id={"seq": me + 2 * way}, device_id_type=MESH)

    @pl.loop(0, coarse.shape[0])
    def _(pair):
        coarse[pair] = jnp.zeros(coarse.shape[1:], jnp.bfloat16)

    pl.semaphore_wait(barrier, 1 + inside(1).astype(jnp.int32) + inside(-1).astype(jnp.int32))

    @pl.loop(0, chunks)
    def _(chunk):
        own_copy(KIND_K, chunk).start()
        own_copy(KIND_V, chunk).start()
        exchange(KIND_K, chunk).start()
        exchange(KIND_V, chunk).start()

        @pl.when(chunk < AHEAD)
        def _():
            start_edge(chunk)

        @pl.when(chunk >= QUERY_LAG)
        def _():
            exchange(KIND_Q, chunk - QUERY_LAG).start()

    @pl.loop(0, chunks)
    def _(chunk):
        own_copy(KIND_Q, chunk).start()

        @pl.when(chunk >= chunks - QUERY_LAG)
        def _():
            exchange(KIND_Q, chunk).start()

    def paired(slot, first, rows, stride, step):
        low = stage[slot, pl.ds(first + step, rows, stride=stride)]
        high = stage[slot, pl.ds(first + step + 1, rows, stride=stride)]
        return (0.5 * (low + high)).astype(jnp.bfloat16)

    def twos_of(slot, first, rows):
        return paired(slot, first, rows // 2, 2, 0)

    def fours_of(slot, first, rows):
        low, high = (paired(slot, first, rows // 4, 4, step).astype(jnp.float32) for step in (0, 2))
        return (0.5 * (low + high)).astype(jnp.bfloat16)

    def pool_half(chunk, half, base=0):
        first = half * rows_dev
        for side in range(2):
            rows = fine[chunk, side, pl.ds(pl.multiple_of(BLOCK + first, BLOCK), rows_dev)]
            stage[base + side] = rows.astype(jnp.float32)
        for side in range(2):
            twos = twos_of(base + side, 0, rows_dev)
            mid[chunk, side, pl.ds(pl.multiple_of(-MID_LOW * HALF + first // 2, HALF), rows_dev // 2)] = twos
            fours = fours_of(base + side, 0, rows_dev)
            far[chunk, side, pl.ds(pl.multiple_of(-FAR_LOW * QUARTER + first // 4, QUARTER), rows_dev // 4)] = fours

    def prepare(chunk):
        await_bytes(fine.at[chunk, :, pl.ds(BLOCK + own_first, rows_dev)], local.at[chunk, 0])
        pool_half(chunk, parity)
        for way in (-1, 1):
            @pl.when(inside(way))
            def _():
                mid_copy(0, way, chunk).start()

                @pl.when(outward == -way)
                def _():
                    far_copy(way, chunk).start()

    @pl.loop(0, AHEAD)
    def _(chunk):
        prepare(chunk)

    for way in (1, -1):
        @pl.when(inside(-way))
        def _():
            pl.semaphore_wait(entered.at[(1 - way) // 2], 1)

        @pl.when(inside(way))
        def _():
            pl.semaphore_signal(
                entered.at[(1 - way) // 2], inc=1, device_id={"seq": me + 2 * way}, device_id_type=MESH
            )

    for window, unit, low, offset, landing, count in (
        (fine, BLOCK, FINE_LOW, 1, -1, 1),
        (fine, BLOCK, FINE_LOW, -1, 4, 1),
        (mid, HALF, MID_LOW, 1, -3, 2),
        (mid, HALF, MID_LOW, -1, 5, 2),
        (far, QUARTER, FAR_LOW, 1, -4, 1),
        (far, QUARTER, FAR_LOW, -1, 7, 1),
        (far, QUARTER, FAR_LOW, 2, -8, 4),
        (far, QUARTER, FAR_LOW, -2, 8, 4),
        (far, QUARTER, FAR_LOW, 3, -9, 1),
        (far, QUARTER, FAR_LOW, -3, 12, 1),
    ):
        @pl.when(jnp.logical_not(inside(-offset)))
        def _():
            @pl.loop(0, chunks)
            def _(chunk):
                window[chunk, :, pl.ds((landing - low) * unit, count * unit)] = jnp.zeros(
                    (2, count * unit, HEAD_DIM), jnp.bfloat16
                )

    atoms = bias.shape[1]
    total_blocks = groups * GROUP_BLOCKS
    place = lax.broadcasted_iota(jnp.int32, (1, atoms), 1)
    windows_end = 8 * BLOCK
    for block in range(GROUP_BLOCKS):
        rel = jnp.where(
            place < 384,
            block - 1 + place // BLOCK,
            jnp.where(
                place < 512,
                block - 3 + (place - 384) // HALF,
                jnp.where(
                    place < 640,
                    block + 2 + (place - 512) // HALF,
                    jnp.where(
                        place < 832,
                        block - 9 + (place - 640) // QUARTER,
                        block + 4 + (place - 832) // QUARTER,
                    ),
                ),
            ),
        )
        here = group * GROUP_BLOCKS + rel
        held = (here >= 0) & (here < total_blocks)
        late = place - windows_end
        slot_row = late % COARSE_SLOT
        slot = late // COARSE_SLOT
        giver = jnp.where(slot < 2, group + 4 * slot - 2, slot - 2)
        given = (giver >= 0) & (giver < groups) & ((slot < 2) | (jnp.abs(giver - group) > 2))
        coarse_block = giver * GROUP_BLOCKS + slot_row % COARSE_USED * POOL // BLOCK
        apart = jnp.abs(coarse_block - (group * GROUP_BLOCKS + block)) > FAR_REACH
        log_size = jnp.where(
            place < 384, 0.0, jnp.where(place < 640, 1.0, jnp.where(place < windows_end, 2.0, math.log2(POOL)))
        )
        for odd in range(2):
            used = slot_row // COARSE_USED == jnp.where(slot < 2, 0, odd)
            allowed = ((place < windows_end) & held) | ((place >= windows_end) & used & given & apart)
            bias[odd * GROUP_BLOCKS + block : odd * GROUP_BLOCKS + block + 1, :] = jnp.where(
                allowed, log_size, -jnp.inf
            )

    def near_coarse(chunk, side, offset):
        first = (offset * GROUP_BLOCKS - FAR_LOW) * QUARTER
        return pooled(far[chunk, side, first : first + GROUP_ROWS // 4], COARSE_SLOT, POOL // 4)

    def gather(chunk):
        await_bytes(fine.at[chunk, :, pl.ds(BLOCK + other_first, rows_dev)], recv.at[chunk, RECV_OF[KIND_K]])

        @pl.when(inside(-outward))
        def _():
            fine_copy(chunk).start()

        pool_half(chunk, 1 - parity)
        for way in (-1, 1):
            @pl.when(inside(way))
            def _():
                mid_copy(1, way, chunk).start()

                @pl.when(outward == way)
                def _():
                    far_copy(way, chunk).start()

        start_routes(DIRECT, chunk)

        @pl.when((inside(3) | inside(-3)) & (chunk % 2 == 1))
        def _():
            slot = pl.ds(pl.multiple_of(group * COARSE_SLOT, COARSE_SLOT), COARSE_SLOT)
            pair = chunk // 2
            own = far_rows(0, GROUP_BLOCKS)
            for side in range(2):
                fours = jnp.concatenate([far[chunk - 1, side, own], far[chunk, side, own]], axis=0)
                coarse[pair, side, slot] = pooled(fours, COARSE_SLOT, POOL // 4)

            @pl.loop(1, groups)
            def _(step):
                @pl.when(jnp.abs(lax.rem(group + step, groups) - group) > 2)
                def _():
                    coarse_copy(pair, step).start()

    def relay(chunk):
        @pl.when(inside(-outward))
        def _():
            await_bytes(fine.at[chunk, :, :BLOCK], recv.at[chunk, RECV_OF[KIND_EDGE_K]])

        @pl.when(inside(outward))
        def _():
            fine_copy(chunk).wait_recv()

        for way in (-1, 1):
            @pl.when(inside(-way))
            def _():
                await_bytes(
                    far.at[chunk, :, : 2 * HALF + QUARTER], recv.at[chunk, RECV_OF[KIND_FAR + (way < 0)]]
                )

        for side in range(2):
            for end, near_mid in ((0, 0), (GROUP_BLOCKS + 1, GROUP_BLOCKS + MID_REACH + 1)):
                slot = 2 * side + (end > 0)
                stage[slot, :BLOCK] = fine[chunk, side, end * BLOCK : (end + 1) * BLOCK].astype(jnp.float32)
                stage[slot, BLOCK:] = mid[chunk, side, near_mid * HALF : (near_mid + 2) * HALF].astype(jnp.float32)
        for side in range(2):
            for end, one, two in ((0, -1, -3), (1, GROUP_BLOCKS, GROUP_BLOCKS + 1)):
                slot = 2 * side + end
                mid[chunk, side, mid_rows(one)] = twos_of(slot, 0, BLOCK)
                far[chunk, side, far_rows(one, 1)] = fours_of(slot, 0, BLOCK)
                far[chunk, side, far_rows(two, 2)] = twos_of(slot, BLOCK, BLOCK)
        start_routes(SECOND_HOP, chunk)

    scale = math.log2(math.e) / math.sqrt(HEAD_DIM)

    def rows_at(ref, chunk, side, first, count, unit):
        return ref[chunk, side, pl.ds(pl.multiple_of(first * unit, unit), count * unit)]

    def attend(chunk):
        own_copy(KIND_Q, chunk).wait()
        exchange(KIND_Q, chunk).wait_recv()
        await_routes(SECOND_HOP + DIRECT, chunk)

        pair = chunk // 2

        @pl.when((inside(3) | inside(-3)) & (chunk % 2 == 0))
        def _():
            @pl.loop(1, groups)
            def _(step):
                giver = lax.rem(group - step + groups, groups)
                origin = pl.ds(pl.multiple_of(giver * COARSE_SLOT, COARSE_SLOT), COARSE_SLOT)

                @pl.when(jnp.abs(giver - group) > 2)
                def _():
                    pltpu.make_async_remote_copy(
                        src_ref=coarse.at[pair, :, origin], dst_ref=coarse.at[pair, :, origin],
                        send_sem=coarse_send.at[pair, step], recv_sem=coarse_recv.at[pair, step],
                        device_id={"seq": partner}, device_id_type=MESH,
                    ).wait_recv()

        near = [[near_coarse(chunk, side, offset) for offset in (-2, 2)] for side in range(2)]

        def atom_rows(block, side):
            return jnp.concatenate(
                [
                    rows_at(fine, chunk, side, block, 3, BLOCK),
                    rows_at(mid, chunk, side, block, 2, HALF),
                    rows_at(mid, chunk, side, block + 5, 2, HALF),
                    rows_at(far, chunk, side, block, 6, QUARTER),
                    rows_at(far, chunk, side, block + 13, 6, QUARTER),
                    *near[side],
                    coarse[pair, side],
                ],
                axis=0,
            )

        def score_block(block):
            here = pl.ds(pl.multiple_of(block * BLOCK, BLOCK), BLOCK)
            return lax.dot_general(
                q_rows[chunk, here], atom_rows(block, 0),
                (((1,), (1,)), ((), ())), preferred_element_type=jnp.float32,
            ) * scale + bias[pl.ds(chunk % 2 * GROUP_BLOCKS + block, 1), :]

        def finish_block(block, scores):
            here = pl.ds(pl.multiple_of(block * BLOCK, BLOCK), BLOCK)
            row_top = jnp.max(scores, axis=1, keepdims=True)
            exp_terms = jnp.exp2(scores - row_top)
            denominator = jnp.sum(exp_terms, axis=1, keepdims=True)
            weighted = jnp.dot(
                exp_terms.astype(jnp.bfloat16), atom_rows(block, 1), preferred_element_type=jnp.float32
            )
            out_rows[chunk, here] = (weighted / denominator).astype(jnp.bfloat16)

        theirs = [(1 - parity) * half_blocks + step for step in range(half_blocks)]
        ours = [parity * half_blocks + step for step in range(half_blocks)]
        order = theirs + ours
        scores = [score_block(order[0]), score_block(order[1])]
        for step in range(GROUP_BLOCKS):
            if step + 2 < GROUP_BLOCKS:
                scores.append(score_block(order[step + 2]))
            finish_block(order[step], scores[step])
            if step < half_blocks:
                result_copy(step, chunk).start()
        own_result(chunk).start()

    def look_ahead(chunk):
        @pl.when(chunk + AHEAD < chunks)
        def _():
            start_edge(chunk + AHEAD)
            prepare(chunk + AHEAD)

    stages = ((gather, 0), (look_ahead, 0), (relay, RELAY_LAG), (attend, ATTEND_LAG))

    @pl.loop(0, chunks + ATTEND_LAG)
    def _(step):
        for stage, lag in stages:
            @pl.when((step >= lag) & (step < chunks + lag))
            def _():
                stage(step - lag)

    for kind in (KIND_K, KIND_V, KIND_Q):
        exchange(kind, ALL).wait_send()

    @pl.when(inside(outward))
    def _():
        edge_copy(0, ALL).wait_send()
        edge_copy(1, ALL).wait_send()

    @pl.when(inside(-outward))
    def _():
        fine_copy(ALL).wait_send()

    for way in (-1, 1):
        @pl.when(inside(way))
        def _():
            mid_copy(0, way, ALL).wait_send()
            mid_copy(1, way, ALL).wait_send()
            far_copy(way, ALL).wait_send()

    for route in SECOND_HOP + DIRECT:
        @pl.when(inside(route[5]) & inside(route[5] - route[1]))
        def _():
            routed(route, ALL).wait_send()

    @pl.loop(0, chunks // 2)
    def _(pair):
        @pl.loop(1, groups)
        def _(step):
            @pl.when(jnp.abs(lax.rem(group + step, groups) - group) > 2)
            def _():
                coarse_copy(pair, step).wait_send()

    whole = q_rows.at[:, pl.ds(own_first, rows_dev)]
    await_bytes(whole, result_recv.at[2])
    for step in range(half_blocks):
        result_copy(step, ALL).wait_send()
        result_copy(step, ALL).wait_recv()


def per_device(queries, key_rows, value_rows):
    rows_dev, cols = queries.shape
    groups = lax.axis_size("seq") // 2
    chunks = cols // 2 // HEAD_DIM
    atoms = 8 * BLOCK + (groups + 2) * COARSE_SLOT
    bf16 = jnp.bfloat16
    placed = pl.BlockSpec(memory_space=pltpu.HBM)
    return pl.pallas_call(
        functools.partial(kernel, groups),
        out_shape=jax.ShapeDtypeStruct(queries.shape, bf16),
        in_specs=[placed] * 3,
        out_specs=placed,
        scratch_shapes=[
            pltpu.VMEM((chunks, 2 * rows_dev, HEAD_DIM), bf16),
            pltpu.VMEM((chunks, 2, FINE_BLOCKS * BLOCK, HEAD_DIM), bf16),
            pltpu.VMEM((chunks, 2, MID_BLOCKS * HALF, HEAD_DIM), bf16),
            pltpu.VMEM((chunks, 2, FAR_BLOCKS * QUARTER, HEAD_DIM), bf16),
            pltpu.VMEM((chunks // 2, 2, groups * COARSE_SLOT, HEAD_DIM), bf16),
            pltpu.VMEM((chunks, 2 * rows_dev, HEAD_DIM), bf16),
            pltpu.VMEM((2 * GROUP_BLOCKS, atoms), jnp.float32),
            pltpu.VMEM((STAGES, rows_dev, HEAD_DIM), jnp.float32),
            pltpu.SemaphoreType.DMA((KINDS,)),
            pltpu.SemaphoreType.DMA((chunks, RECV_KINDS)),
            pltpu.SemaphoreType.DMA((3,)),
            pltpu.SemaphoreType.DMA((chunks // 2, groups)),
            pltpu.SemaphoreType.DMA((chunks // 2, groups)),
            pltpu.SemaphoreType.DMA((chunks, 2)),
            pltpu.SemaphoreType.REGULAR((2,)),
        ],
        compiler_params=pltpu.CompilerParams(
            collective_id=0, has_side_effects=True, vmem_limit_bytes=48 * 1024 * 1024
        ),
    )(*(pltpu.with_memory_space_constraint(source, pltpu.HBM) for source in (queries, key_rows, value_rows)))


def solution(mesh):
    placed = (P("seq", "head"), P("seq", "head"), P("seq", "head"))
    return jax.shard_map(
        per_device, mesh=mesh, in_specs=placed, out_specs=P("seq", "head"), check_vma=False
    )
```

```python
import functools
import math

import jax
import jax.numpy as jnp
from jax import lax
from jax.experimental import pallas as pl
from jax.experimental.pallas import tpu as pltpu
from jax.sharding import PartitionSpec as P

HEAD_DIM = 128
BLOCK = 128
POOL = 64
MID_REACH = 3
FAR_REACH = 9

HALF = BLOCK // 2
QUARTER = BLOCK // 4
GROUP_BLOCKS = 4
GROUP_ROWS = GROUP_BLOCKS * BLOCK
COARSE_SLOT = 16
COARSE_USED = GROUP_ROWS // POOL

FINE_LOW, FINE_BLOCKS = -1, GROUP_BLOCKS + 2
MID_LOW, MID_BLOCKS = -MID_REACH, GROUP_BLOCKS + 2 * MID_REACH
FAR_LOW, FAR_BLOCKS = -FAR_REACH, GROUP_BLOCKS + 2 * FAR_REACH

KIND_K, KIND_V, KIND_Q, KIND_BACK, KIND_EDGE_K, KIND_EDGE_V, KIND_FINE, KIND_MID_OWN = range(8)
KIND_MID_OTHER, KIND_FAR = KIND_MID_OWN + 2, KIND_MID_OWN + 4
SECOND_HOP = (
    (13, 2, -4, 4, -8, 1),
    (14, -2, 4, 4, 8, -1),
)
DIRECT = (
    (15, 3, 3, 1, -9, 3),
    (KIND_BACK, -3, 0, 1, 12, -3),
)
RELAY_LAG, ATTEND_LAG = 2, 4
AHEAD, QUERY_LAG = 4, 2
STAGES = 4
RECV_OF = (0, 0, 1, 2, 3, 3, 4, 5, 6, 5, 6, 5, 6, 7, 8, 9)
RECV_KINDS, KINDS = 10, 18
KIND_O, KIND_LAST = 16, 17
ALL = slice(None)
MESH = pl.DeviceIdType.MESH


def pool_matrix(out_rows, in_rows, group_rows):
    row = lax.broadcasted_iota(jnp.int32, (out_rows, in_rows), 0)
    col = lax.broadcasted_iota(jnp.int32, (out_rows, in_rows), 1)
    return jnp.where(col // group_rows == row, 1.0 / group_rows, 0.0).astype(jnp.bfloat16)


def pooled(source, out_rows, group_rows):
    weights = pool_matrix(out_rows, source.shape[0], group_rows)
    return jnp.dot(weights, source, preferred_element_type=jnp.float32).astype(jnp.bfloat16)


def kernel(
    groups, q_ref, k_ref, v_ref, o_ref,
    q_rows, fine, mid, far, coarse, out_rows, bias,
    stage, send, recv, result_recv, coarse_send, coarse_recv, local, entered,
):
    me = lax.axis_index("seq")
    group = me // 2
    parity = me % 2
    partner = me + 1 - 2 * parity
    outward = 2 * parity - 1
    rows_dev = q_ref.shape[0]
    chunks = q_rows.shape[0]
    half_cols = chunks * HEAD_DIM
    own_first = pl.multiple_of(parity * rows_dev, rows_dev)
    other_first = pl.multiple_of((1 - parity) * rows_dev, rows_dev)
    half_blocks = GROUP_BLOCKS // 2

    def own_cols(chunk):
        if chunk is ALL:
            return pl.ds(pl.multiple_of(parity * half_cols, HEAD_DIM), half_cols)
        return pl.ds(pl.multiple_of(parity * half_cols + chunk * HEAD_DIM, HEAD_DIM), HEAD_DIM)

    def other_cols(chunk):
        if chunk is ALL:
            return pl.ds(pl.multiple_of((1 - parity) * half_cols, HEAD_DIM), half_cols)
        return pl.ds(pl.multiple_of((1 - parity) * half_cols + chunk * HEAD_DIM, HEAD_DIM), HEAD_DIM)

    def fine_rows(block):
        return pl.ds(pl.multiple_of((block - FINE_LOW) * BLOCK, BLOCK), BLOCK)

    def remote(src, dst, kind, chunk, target):
        if kind in (KIND_O, KIND_LAST):
            arrived = result_recv.at[kind - KIND_O]
        else:
            arrived = recv.at[0 if chunk is ALL else chunk, RECV_OF[kind]]
        return pltpu.make_async_remote_copy(
            src_ref=src, dst_ref=dst, send_sem=send.at[kind], recv_sem=arrived,
            device_id={"seq": target}, device_id_type=MESH,
        )

    def exchange(kind, chunk):
        if kind == KIND_Q:
            return remote(
                q_ref.at[:, other_cols(chunk)], q_rows.at[chunk, pl.ds(own_first, rows_dev)],
                kind, chunk, partner,
            )
        source = k_ref if kind == KIND_K else v_ref
        return remote(
            source.at[:, other_cols(chunk)], fine.at[chunk, kind, pl.ds(BLOCK + own_first, rows_dev)],
            kind, chunk, partner,
        )

    def result_copy(step, chunk):
        source = out_rows.at[chunk, pl.ds(pl.multiple_of(other_first + step * BLOCK, BLOCK), BLOCK)]
        return remote(
            source, o_ref.at[step * BLOCK : (step + 1) * BLOCK, own_cols(chunk)], KIND_O + step * (KIND_LAST - KIND_O),
            chunk, partner,
        )

    def edge_copy(side, chunk):
        source = v_ref if side else k_ref
        rows = pl.ds(pl.multiple_of(parity * (rows_dev - BLOCK), BLOCK), BLOCK)
        landing = (1 - parity) * (GROUP_BLOCKS + 1) - 1
        return remote(
            source.at[rows, own_cols(chunk)], fine.at[chunk, side, fine_rows(landing)],
            KIND_EDGE_K + side, chunk, me + 2 * outward,
        )

    def fine_copy(chunk):
        first = (1 - parity) * (GROUP_BLOCKS - 1)
        landing = parity * (GROUP_BLOCKS + 1) - 1
        return remote(
            fine.at[chunk, :, fine_rows(first)], fine.at[chunk, :, fine_rows(landing)],
            KIND_FINE, chunk, me - 2 * outward,
        )

    def mid_rows(block):
        return pl.ds(pl.multiple_of((block - MID_LOW) * HALF, HALF), HALF)

    def far_rows(first, count):
        return pl.ds((first - FAR_LOW) * QUARTER, count * QUARTER)

    def mid_copy(other, way, chunk):
        block = 2 - parity if other else 1 + parity
        return remote(
            mid.at[chunk, :, mid_rows(block)], mid.at[chunk, :, mid_rows(block - GROUP_BLOCKS * way)],
            KIND_MID_OWN + 2 * other + (way < 0), chunk, me + 2 * way,
        )

    def far_copy(way, chunk):
        first, landing = (0, -GROUP_BLOCKS) if way > 0 else (GROUP_BLOCKS - 1, 2 * GROUP_BLOCKS - 1)
        return remote(
            far.at[chunk, :, far_rows(first, 1)], far.at[chunk, :, far_rows(landing, 1)],
            KIND_FAR + (way < 0), chunk, me + 2 * way,
        )

    def routed(route, chunk):
        kind, offset, first, count, landing, hop = route
        return remote(
            far.at[chunk, :, far_rows(first, count)], far.at[chunk, :, far_rows(landing, count)],
            kind, chunk, me + 2 * hop,
        )

    def coarse_copy(pair, step):
        target = lax.rem(group + step, groups) * 2 + parity
        slot = pl.ds(pl.multiple_of(group * COARSE_SLOT, COARSE_SLOT), COARSE_SLOT)
        return pltpu.make_async_remote_copy(
            src_ref=coarse.at[pair, :, slot], dst_ref=coarse.at[pair, :, slot],
            send_sem=coarse_send.at[step], recv_sem=coarse_recv.at[pair, step],
            device_id={"seq": target}, device_id_type=MESH,
        )

    def await_bytes(ref, semaphore):
        pltpu.make_async_copy(ref, ref, semaphore).wait()

    def inside(offset):
        return (group + offset >= 0) & (group + offset < groups)

    def start_routes(routes, chunk):
        for route in routes:
            @pl.when(inside(route[5]) & inside(route[5] - route[1]))
            def _():
                routed(route, chunk).start()

    def await_routes(routes, chunk):
        for route in routes:
            @pl.when(inside(-route[1]))
            def _():
                routed(route, chunk).wait_recv()

    def own_copy(kind, chunk):
        if kind == KIND_Q:
            source, target = q_ref, q_rows.at[chunk, pl.ds(own_first, rows_dev)]
        else:
            source = k_ref if kind == KIND_K else v_ref
            target = fine.at[chunk, kind, pl.ds(BLOCK + own_first, rows_dev)]
        return pltpu.make_async_copy(source.at[:, own_cols(chunk)], target, local.at[chunk, kind // 2])

    def own_result(chunk):
        return pltpu.make_async_copy(
            out_rows.at[chunk, pl.ds(own_first, rows_dev)], o_ref.at[:, own_cols(chunk)], result_recv.at[2],
        )

    def start_edge(chunk):
        @pl.when(inside(outward))
        def _():
            edge_copy(0, chunk).start()
            edge_copy(1, chunk).start()

    barrier = pltpu.get_barrier_semaphore()
    pl.semaphore_signal(barrier, inc=1, device_id={"seq": partner}, device_id_type=MESH)
    for way in (1, -1):
        @pl.when(inside(way))
        def _():
            pl.semaphore_signal(barrier, inc=1, device_id={"seq": me + 2 * way}, device_id_type=MESH)

    @pl.loop(0, coarse.shape[0])
    def _(pair):
        coarse[pair] = jnp.zeros(coarse.shape[1:], jnp.bfloat16)

    pl.semaphore_wait(barrier, 1 + inside(1).astype(jnp.int32) + inside(-1).astype(jnp.int32))

    @pl.loop(0, chunks)
    def _(chunk):
        own_copy(KIND_K, chunk).start()
        own_copy(KIND_V, chunk).start()
        exchange(KIND_K, chunk).start()
        exchange(KIND_V, chunk).start()

        @pl.when(chunk < AHEAD)
        def _():
            start_edge(chunk)

        @pl.when(chunk >= QUERY_LAG)
        def _():
            exchange(KIND_Q, chunk - QUERY_LAG).start()

    @pl.loop(0, chunks)
    def _(chunk):
        own_copy(KIND_Q, chunk).start()

        @pl.when(chunk >= chunks - QUERY_LAG)
        def _():
            exchange(KIND_Q, chunk).start()

    def paired(slot, first, rows, stride, step):
        low = stage[slot, pl.ds(first + step, rows, stride=stride)]
        high = stage[slot, pl.ds(first + step + 1, rows, stride=stride)]
        return (0.5 * (low + high)).astype(jnp.bfloat16)

    def twos_of(slot, first, rows):
        return paired(slot, first, rows // 2, 2, 0)

    def fours_of(slot, first, rows):
        low, high = (paired(slot, first, rows // 4, 4, step).astype(jnp.float32) for step in (0, 2))
        return (0.5 * (low + high)).astype(jnp.bfloat16)

    def pool_half(chunk, half, base=0):
        first = half * rows_dev
        for side in range(2):
            rows = fine[chunk, side, pl.ds(pl.multiple_of(BLOCK + first, BLOCK), rows_dev)]
            stage[base + side] = rows.astype(jnp.float32)
        for side in range(2):
            twos = twos_of(base + side, 0, rows_dev)
            mid[chunk, side, pl.ds(pl.multiple_of(-MID_LOW * HALF + first // 2, HALF), rows_dev // 2)] = twos
            fours = fours_of(base + side, 0, rows_dev)
            far[chunk, side, pl.ds(pl.multiple_of(-FAR_LOW * QUARTER + first // 4, QUARTER), rows_dev // 4)] = fours

    def prepare(chunk):
        await_bytes(fine.at[chunk, :, pl.ds(BLOCK + own_first, rows_dev)], local.at[chunk, 0])
        pool_half(chunk, parity)
        for way in (-1, 1):
            @pl.when(inside(way))
            def _():
                mid_copy(0, way, chunk).start()

                @pl.when(outward == -way)
                def _():
                    far_copy(way, chunk).start()

    @pl.loop(0, AHEAD)
    def _(chunk):
        prepare(chunk)

    for way in (1, -1):
        @pl.when(inside(-way))
        def _():
            pl.semaphore_wait(entered.at[(1 - way) // 2], 1)

        @pl.when(inside(way))
        def _():
            pl.semaphore_signal(
                entered.at[(1 - way) // 2], inc=1, device_id={"seq": me + 2 * way}, device_id_type=MESH
            )

    for window, unit, low, offset, landing, count in (
        (fine, BLOCK, FINE_LOW, 1, -1, 1),
        (fine, BLOCK, FINE_LOW, -1, 4, 1),
        (mid, HALF, MID_LOW, 1, -3, 2),
        (mid, HALF, MID_LOW, -1, 5, 2),
        (far, QUARTER, FAR_LOW, 1, -4, 1),
        (far, QUARTER, FAR_LOW, -1, 7, 1),
        (far, QUARTER, FAR_LOW, 2, -8, 4),
        (far, QUARTER, FAR_LOW, -2, 8, 4),
        (far, QUARTER, FAR_LOW, 3, -9, 1),
        (far, QUARTER, FAR_LOW, -3, 12, 1),
    ):
        @pl.when(jnp.logical_not(inside(-offset)))
        def _():
            @pl.loop(0, chunks)
            def _(chunk):
                window[chunk, :, pl.ds((landing - low) * unit, count * unit)] = jnp.zeros(
                    (2, count * unit, HEAD_DIM), jnp.bfloat16
                )

    atoms = bias.shape[1]
    total_blocks = groups * GROUP_BLOCKS
    place = lax.broadcasted_iota(jnp.int32, (1, atoms), 1)
    windows_end = 8 * BLOCK
    for block in range(GROUP_BLOCKS):
        rel = jnp.where(
            place < 384,
            block - 1 + place // BLOCK,
            jnp.where(
                place < 512,
                block - 3 + (place - 384) // HALF,
                jnp.where(
                    place < 640,
                    block + 2 + (place - 512) // HALF,
                    jnp.where(
                        place < 832,
                        block - 9 + (place - 640) // QUARTER,
                        block + 4 + (place - 832) // QUARTER,
                    ),
                ),
            ),
        )
        here = group * GROUP_BLOCKS + rel
        held = (here >= 0) & (here < total_blocks)
        late = place - windows_end
        slot_row = late % COARSE_SLOT
        slot = late // COARSE_SLOT
        giver = jnp.where(slot < 2, group + 4 * slot - 2, slot - 2)
        given = (giver >= 0) & (giver < groups) & ((slot < 2) | (jnp.abs(giver - group) > 2))
        coarse_block = giver * GROUP_BLOCKS + slot_row % COARSE_USED * POOL // BLOCK
        apart = jnp.abs(coarse_block - (group * GROUP_BLOCKS + block)) > FAR_REACH
        log_size = jnp.where(
            place < 384, 0.0, jnp.where(place < 640, 1.0, jnp.where(place < windows_end, 2.0, math.log2(POOL)))
        )
        for odd in range(2):
            used = slot_row // COARSE_USED == jnp.where(slot < 2, 0, odd)
            allowed = ((place < windows_end) & held) | ((place >= windows_end) & used & given & apart)
            bias[odd * GROUP_BLOCKS + block : odd * GROUP_BLOCKS + block + 1, :] = jnp.where(
                allowed, log_size, -jnp.inf
            )

    def near_coarse(chunk, side, offset):
        first = (offset * GROUP_BLOCKS - FAR_LOW) * QUARTER
        return pooled(far[chunk, side, first : first + GROUP_ROWS // 4], COARSE_SLOT, POOL // 4)

    def gather(chunk):
        await_bytes(fine.at[chunk, :, pl.ds(BLOCK + other_first, rows_dev)], recv.at[chunk, RECV_OF[KIND_K]])

        @pl.when(inside(-outward))
        def _():
            fine_copy(chunk).start()

        pool_half(chunk, 1 - parity)
        for way in (-1, 1):
            @pl.when(inside(way))
            def _():
                mid_copy(1, way, chunk).start()

                @pl.when(outward == way)
                def _():
                    far_copy(way, chunk).start()

        start_routes(DIRECT, chunk)

        @pl.when((inside(3) | inside(-3)) & (chunk % 2 == 1))
        def _():
            slot = pl.ds(pl.multiple_of(group * COARSE_SLOT, COARSE_SLOT), COARSE_SLOT)
            pair = chunk // 2
            own = far_rows(0, GROUP_BLOCKS)
            for side in range(2):
                fours = jnp.concatenate([far[chunk - 1, side, own], far[chunk, side, own]], axis=0)
                coarse[pair, side, slot] = pooled(fours, COARSE_SLOT, POOL // 4)

            @pl.loop(1, groups)
            def _(step):
                @pl.when(jnp.abs(lax.rem(group + step, groups) - group) > 2)
                def _():
                    coarse_copy(pair, step).start()

    def relay(chunk):
        @pl.when(inside(-outward))
        def _():
            await_bytes(fine.at[chunk, :, :BLOCK], recv.at[chunk, RECV_OF[KIND_EDGE_K]])

        @pl.when(inside(outward))
        def _():
            fine_copy(chunk).wait_recv()

        for way in (-1, 1):
            @pl.when(inside(-way))
            def _():
                await_bytes(
                    far.at[chunk, :, : 2 * HALF + QUARTER], recv.at[chunk, RECV_OF[KIND_FAR + (way < 0)]]
                )

        for side in range(2):
            for end, near_mid in ((0, 0), (GROUP_BLOCKS + 1, GROUP_BLOCKS + MID_REACH + 1)):
                slot = 2 * side + (end > 0)
                stage[slot, :BLOCK] = fine[chunk, side, end * BLOCK : (end + 1) * BLOCK].astype(jnp.float32)
                stage[slot, BLOCK:] = mid[chunk, side, near_mid * HALF : (near_mid + 2) * HALF].astype(jnp.float32)
        for side in range(2):
            for end, one, two in ((0, -1, -3), (1, GROUP_BLOCKS, GROUP_BLOCKS + 1)):
                slot = 2 * side + end
                mid[chunk, side, mid_rows(one)] = twos_of(slot, 0, BLOCK)
                far[chunk, side, far_rows(one, 1)] = fours_of(slot, 0, BLOCK)
                far[chunk, side, far_rows(two, 2)] = twos_of(slot, BLOCK, BLOCK)
        start_routes(SECOND_HOP, chunk)

    scale = math.log2(math.e) / math.sqrt(HEAD_DIM)

    def rows_at(ref, chunk, side, first, count, unit):
        return ref[chunk, side, pl.ds(pl.multiple_of(first * unit, unit), count * unit)]

    def attend(chunk):
        own_copy(KIND_Q, chunk).wait()
        exchange(KIND_Q, chunk).wait_recv()
        await_routes(SECOND_HOP + DIRECT, chunk)

        pair = chunk // 2

        @pl.when((inside(3) | inside(-3)) & (chunk % 2 == 0))
        def _():
            @pl.loop(1, groups)
            def _(step):
                giver = lax.rem(group - step + groups, groups)
                origin = pl.ds(pl.multiple_of(giver * COARSE_SLOT, COARSE_SLOT), COARSE_SLOT)

                @pl.when(jnp.abs(giver - group) > 2)
                def _():
                    pltpu.make_async_remote_copy(
                        src_ref=coarse.at[pair, :, origin], dst_ref=coarse.at[pair, :, origin],
                        send_sem=coarse_send.at[step], recv_sem=coarse_recv.at[pair, step],
                        device_id={"seq": partner}, device_id_type=MESH,
                    ).wait_recv()

        near = [[near_coarse(chunk, side, offset) for offset in (-2, 2)] for side in range(2)]

        def atom_rows(block, side):
            return jnp.concatenate(
                [
                    rows_at(fine, chunk, side, block, 3, BLOCK),
                    rows_at(mid, chunk, side, block, 2, HALF),
                    rows_at(mid, chunk, side, block + 5, 2, HALF),
                    rows_at(far, chunk, side, block, 6, QUARTER),
                    rows_at(far, chunk, side, block + 13, 6, QUARTER),
                    *near[side],
                    coarse[pair, side],
                ],
                axis=0,
            )

        def score_block(block):
            here = pl.ds(pl.multiple_of(block * BLOCK, BLOCK), BLOCK)
            return lax.dot_general(
                q_rows[chunk, here], atom_rows(block, 0),
                (((1,), (1,)), ((), ())), preferred_element_type=jnp.float32,
            ) * scale + bias[pl.ds(chunk % 2 * GROUP_BLOCKS + block, 1), :]

        def finish_block(block, scores):
            here = pl.ds(pl.multiple_of(block * BLOCK, BLOCK), BLOCK)
            row_top = jnp.max(scores, axis=1, keepdims=True)
            exp_terms = jnp.exp2(scores - row_top)
            denominator = jnp.sum(exp_terms, axis=1, keepdims=True)
            weighted = jnp.dot(
                exp_terms.astype(jnp.bfloat16), atom_rows(block, 1), preferred_element_type=jnp.float32
            )
            out_rows[chunk, here] = (weighted / denominator).astype(jnp.bfloat16)

        theirs = [(1 - parity) * half_blocks + step for step in range(half_blocks)]
        ours = [parity * half_blocks + step for step in range(half_blocks)]
        order = theirs + ours
        scores = [score_block(order[0]), score_block(order[1])]
        for step in range(GROUP_BLOCKS):
            if step + 2 < GROUP_BLOCKS:
                scores.append(score_block(order[step + 2]))
            finish_block(order[step], scores[step])
            if step < half_blocks:
                result_copy(step, chunk).start()
        own_result(chunk).start()

    def look_ahead(chunk):
        @pl.when(chunk + AHEAD < chunks)
        def _():
            start_edge(chunk + AHEAD)
            prepare(chunk + AHEAD)

    stages = ((gather, 0), (look_ahead, 0), (relay, RELAY_LAG), (attend, ATTEND_LAG))

    @pl.loop(0, chunks + ATTEND_LAG)
    def _(step):
        for stage, lag in stages:
            @pl.when((step >= lag) & (step < chunks + lag))
            def _():
                stage(step - lag)

    for kind in (KIND_K, KIND_V, KIND_Q):
        exchange(kind, ALL).wait_send()

    @pl.when(inside(outward))
    def _():
        edge_copy(0, ALL).wait_send()
        edge_copy(1, ALL).wait_send()

    @pl.when(inside(-outward))
    def _():
        fine_copy(ALL).wait_send()

    for way in (-1, 1):
        @pl.when(inside(way))
        def _():
            mid_copy(0, way, ALL).wait_send()
            mid_copy(1, way, ALL).wait_send()
            far_copy(way, ALL).wait_send()

    for route in SECOND_HOP + DIRECT:
        @pl.when(inside(route[5]) & inside(route[5] - route[1]))
        def _():
            routed(route, ALL).wait_send()

    @pl.loop(1, groups)
    def _(step):
        @pl.when(jnp.abs(lax.rem(group + step, groups) - group) > 2)
        def _():
            pltpu.make_async_remote_copy(
                src_ref=coarse.at[:, :, :COARSE_SLOT], dst_ref=coarse.at[:, :, :COARSE_SLOT],
                send_sem=coarse_send.at[step], recv_sem=coarse_recv.at[0, step],
                device_id={"seq": partner}, device_id_type=MESH,
            ).wait_send()

    whole = q_rows.at[:, pl.ds(own_first, rows_dev)]
    await_bytes(whole, result_recv.at[2])
    for step in range(half_blocks):
        result_copy(step, ALL).wait_send()
        result_copy(step, ALL).wait_recv()


def per_device(queries, key_rows, value_rows):
    rows_dev, cols = queries.shape
    groups = lax.axis_size("seq") // 2
    chunks = cols // 2 // HEAD_DIM
    atoms = 8 * BLOCK + (groups + 2) * COARSE_SLOT
    bf16 = jnp.bfloat16
    placed = pl.BlockSpec(memory_space=pltpu.HBM)
    return pl.pallas_call(
        functools.partial(kernel, groups),
        out_shape=jax.ShapeDtypeStruct(queries.shape, bf16),
        in_specs=[placed] * 3,
        out_specs=placed,
        scratch_shapes=[
            pltpu.VMEM((chunks, 2 * rows_dev, HEAD_DIM), bf16),
            pltpu.VMEM((chunks, 2, FINE_BLOCKS * BLOCK, HEAD_DIM), bf16),
            pltpu.VMEM((chunks, 2, MID_BLOCKS * HALF, HEAD_DIM), bf16),
            pltpu.VMEM((chunks, 2, FAR_BLOCKS * QUARTER, HEAD_DIM), bf16),
            pltpu.VMEM((chunks // 2, 2, groups * COARSE_SLOT, HEAD_DIM), bf16),
            pltpu.VMEM((chunks, 2 * rows_dev, HEAD_DIM), bf16),
            pltpu.VMEM((2 * GROUP_BLOCKS, atoms), jnp.float32),
            pltpu.VMEM((STAGES, rows_dev, HEAD_DIM), jnp.float32),
            pltpu.SemaphoreType.DMA((KINDS,)),
            pltpu.SemaphoreType.DMA((chunks, RECV_KINDS)),
            pltpu.SemaphoreType.DMA((3,)),
            pltpu.SemaphoreType.DMA((groups,)),
            pltpu.SemaphoreType.DMA((chunks // 2, groups)),
            pltpu.SemaphoreType.DMA((chunks, 2)),
            pltpu.SemaphoreType.REGULAR((2,)),
        ],
        compiler_params=pltpu.CompilerParams(
            collective_id=0, has_side_effects=True, vmem_limit_bytes=48 * 1024 * 1024
        ),
    )(*(pltpu.with_memory_space_constraint(source, pltpu.HBM) for source in (queries, key_rows, value_rows)))


def solution(mesh):
    placed = (P("seq", "head"), P("seq", "head"), P("seq", "head"))
    return jax.shard_map(
        per_device, mesh=mesh, in_specs=placed, out_specs=P("seq", "head"), check_vma=False
    )
```
